32 devices in a mesh: rep: 1, r: 4 (over z), s: 8 (over x, y, core).
Axes of the slice: x: 2, y: 2, z: 4, core: 2. Of those that a mesh axis runs over, the one named last changes fastest.
Arguments:
- x: bfloat16 [32, 4096, 768], P(('rep', 'r', 's'))
- dy: bfloat16 [32, 4096, 768], P(('rep', 'r', 's'))
- w_gate: bfloat16 [2, 768, 2048], P(None, 's')
- w_up: bfloat16 [2, 768, 2048], P(None, 's')
- w_down: bfloat16 [2, 2048, 768], P(None, 's')
Outputs:
- output 1: bfloat16 [32, 4096, 768], P(('rep', 'r', 's'))
- output 2: bfloat16 [2, 768, 2048], P('rep', 's')
- output 3: bfloat16 [2, 768, 2048], P('rep', 's')
- output 4: bfloat16 [2, 2048, 768], P('rep', 's')
All inputs are finite; a program needn't handle non-finite values.
Results may differ from the reference program's by a relative error of at most 0.018.
Values are sent between devices in bfloat16 or wider.
A program may use at most 2 GiB of HBM per device.

```python
import jax
import jax.numpy as jnp
from jax import lax

SEQUENCES = 32
TOKENS = 4096
D = 768
FF = 2048
LAYERS = 2
NAMES = ("w_gate", "w_up", "w_down")
SHAPES = {"w_gate": (LAYERS, D, FF), "w_up": (LAYERS, D, FF), "w_down": (LAYERS, FF, D)}


def bump(key, n, height):
    away = (jnp.arange(n, dtype=jnp.int32) - jax.random.randint(key, (), 0, n, jnp.int32)) % n
    return jnp.where(away < n // 8, height, 1.0)


def together(key, own, strength):
    shared = jax.random.normal(key, own.shape[1:], jnp.float32)
    return (own + strength * shared) * lax.rsqrt(1 + strength * strength)


def setup_inputs(seed: int = 0, part: int = 0) -> dict:
    kx, kdy, ka, kb, kz, kf, kh, kl, *kw = jax.random.split(jax.random.key(seed), 8 + len(NAMES))
    kx, kdy, ka, kb = (jax.random.fold_in(k, part) for k in (kx, kdy, ka, kb))
    shape = (SEQUENCES, TOKENS, D)
    much_x, much_dy = jax.random.uniform(kz, (2,), jnp.float32, 0.0, 1.0)
    layers = 2.0 ** jax.random.uniform(kl, (LAYERS, 1, 1), jnp.float32, -1.0, 1.0)
    x = together(ka, jax.random.normal(kx, shape, jnp.float32), much_x) * bump(kf, D, 4.0)
    dy = together(kb, jax.random.normal(kdy, shape, jnp.float32), much_dy)
    drawn = {"x": x.astype(jnp.bfloat16), "dy": (dy * (SEQUENCES * TOKENS) ** -0.5).astype(jnp.bfloat16)}
    for key, name in zip(kw, NAMES, strict=True):
        w = jax.random.normal(key, SHAPES[name], jnp.float32) * SHAPES[name][1] ** -0.5
        drawn[name] = (w * {"w_gate": 1.0, "w_up": bump(kh, FF, 4.0), "w_down": layers}[name]).astype(jnp.bfloat16)
    return drawn


def matmul(a, w):
    return jnp.dot(a, w, preferred_element_type=jnp.float32).astype(jnp.bfloat16)


def normed(h):
    wide = h.astype(jnp.float32)
    scale = lax.rsqrt(jnp.mean(wide**2, -1, keepdims=True) + 1e-6)
    return (wide * scale).astype(jnp.bfloat16)


def layer(h, w):
    a = normed(h)
    gate = jnp.dot(a, w["w_gate"], preferred_element_type=jnp.float32)
    up = jnp.dot(a, w["w_up"], preferred_element_type=jnp.float32)
    return h + matmul((jax.nn.silu(gate) * up).astype(jnp.bfloat16), w["w_down"])


def stack(weights, h):
    return lax.scan(lambda h, w: (layer(h, w), None), h, weights)[0]


def reference(x, dy, w_gate, w_up, w_down):
    weights = dict(zip(NAMES, (w_gate, w_up, w_down), strict=True))

    def take(so_far, sequence):
        h, by_y = sequence
        _, back = jax.vjp(stack, weights, h)
        by_weights, by_h = back(by_y)
        return jax.tree.map(lambda total, term: total + term.astype(jnp.float32), so_far, by_weights), by_h

    none_yet = {name: jnp.zeros(w.shape, jnp.float32) for name, w in weights.items()}
    by_weights, by_x = lax.scan(take, none_yet, (x, dy))
    return (by_x, *(by_weights[name].astype(jnp.bfloat16) for name in NAMES))
```

```python
import functools

import jax
import jax.numpy as jnp
from jax import lax
from jax.experimental import pallas as pl
from jax.experimental.pallas import tpu as pltpu
from jax.sharding import PartitionSpec as P

N, D, FF = 4096, 768, 2048
C, NC = 256, 8
WIDE, BOTH = 2 * C, 2 * FF
QUARTER, PIECE, HALF = C // 2, C // 4, C // 8
ROWS = D // NC
UNITS = 24
PER = UNITS // 2
LAST = 17
OTHERS = (1, 2, 3)
T0, T1, T2, T3, T4, T5 = FF, WIDE, FF, WIDE, FF, WIDE
S0, S1, S2, S3, S4, S5 = 4, 2, 4, 2, 4, 2
M3 = 4
f32, bf16 = jnp.float32, jnp.bfloat16
NN = (((1,), (0,)), ((), ()))
NT = (((1,), (1,)), ((), ()))
TN = (((0,), (0,)), ((), ()))
MESH = pl.DeviceIdType.MESH
VMEM, SEM = pltpu.VMEM, pltpu.SemaphoreType.DMA
PAIR = SEM((2,))
local = pltpu.make_async_copy


def dot(a, b, dims=NN):
    return lax.dot_general(a, b, dims, preferred_element_type=f32)


def scale_of(wide):
    return lax.rsqrt(jnp.mean(wide * wide, -1, keepdims=True) + 1e-6)


def normed(h):
    wide = h.astype(f32)
    return (wide * scale_of(wide)).astype(bf16)


def norm_back(h, by_a, by_out):
    wide = h.astype(f32)
    by_a = by_a.astype(bf16).astype(f32)
    scale = scale_of(wide)
    along = jnp.mean(by_a * wide, -1, keepdims=True) * (scale * scale * scale)
    return (by_out.astype(f32) + (by_a * scale - wide * along).astype(bf16).astype(f32)).astype(bf16)


def back(g, u, dp):
    dp = dp.astype(bf16).astype(f32)
    s = jax.nn.sigmoid(g)
    sg = g * s
    return jnp.concatenate([(dp * u * (s + sg * (1 - s))).astype(bf16), (dp * sg).astype(bf16)], 1), sg * u


def times(start, size):
    return pl.ds(pl.multiple_of(start * size, size), size)


def loop(count, body):
    def step(i, carry):
        body(i)
        return carry

    lax.fori_loop(0, count, step, 0)


def fetch(i, count, copies):
    @pl.when(i == 0)
    def _():
        for c in copies(i):
            c.start()

    @pl.when(i + 1 < count)
    def _():
        for c in copies(i + 1):
            c.start()


def arrive(copies):
    for c in copies:
        c.wait()


def again(i, copy):
    pl.when(i >= 2)(copy.wait)


def added(t, ref, term):
    return jnp.where(t == 0, 0.0, ref) + term


def kernel(x, dy, wg, wu, wd, dx, og, od, gus, ps, dgus, h1s, a0s, dws, A, DY, WGU, WD, lsem, go):
    x_in, dy_in = local(x, A, lsem.at[0]), local(dy, DY, lsem.at[1])
    a_out, a_in = local(A, a0s, lsem.at[0]), local(a0s, A, lsem.at[0])
    x_in.start()
    dy_in.start()
    go.open()
    x_in.wait()

    @functools.partial(loop, N // C)
    def _(t):
        A[times(t, C), :] = normed(A[times(t, C), :])

    a_out.start()
    go.weights_first()

    def forward(hid, sp):
        pl.run_scoped(functools.partial(hidden0, hid), VMEM((2, T0, WIDE), f32), PAIR)
        a_out.wait()
        local(hid, ps, sp).start()
        pl.run_scoped(functools.partial(states1, hid), VMEM((2, T1, D), bf16), VMEM((2, T1, D), bf16), PAIR, PAIR)
        local(hid, ps, sp).wait()

    def hidden0(hid, stg, ss):
        B, nt = T0 // S0, N // T0

        def leave(it):
            return local(stg.at[it % 2], gus.at[it // nt, times(it % nt, T0)], ss.at[it % 2])

        def tile(it):
            j, t, slot = it // nt, it % nt, it % 2
            again(it, leave(it))
            go.step0(it)
            w = WGU[0, :, times(j, WIDE)]
            for k in range(S0):
                gu = dot(A[pl.ds(t * T0 + k * B, B), :], w)
                stg[slot, pl.ds(k * B, B)] = gu
                g, u = gu[:, :C], gu[:, C:]
                hid[pl.ds(t * T0 + k * B, B), times(j, C)] = (g * jax.nn.sigmoid(g) * u).astype(bf16)
            leave(it).start()

        loop(NC * nt, tile)
        arrive(map(leave, range(2)))

    def states1(hid, stx, sth, ss, sx):
        B, nt = T1 // S1, N // T1

        def come(t):
            return [local(x.at[times(t, T1)], stx.at[t % 2], sx.at[t % 2])]

        def leave(t):
            return local(sth.at[t % 2], h1s.at[times(t, T1)], ss.at[t % 2])

        def tile(t):
            slot = t % 2
            fetch(t, nt, come)
            again(t, leave(t))
            arrive(come(t))
            go.step1(t)
            for k in range(S1):
                m = dot(hid[pl.ds(t * T1 + k * B, B), :], WD[0]).astype(bf16)
                h = (stx[slot, pl.ds(k * B, B)].astype(f32) + m.astype(f32)).astype(bf16)
                sth[slot, pl.ds(k * B, B)] = h
                A[pl.ds(t * T1 + k * B, B), :] = normed(h)
            leave(t).start()

        loop(nt, tile)
        arrive(map(leave, range(2)))

    pl.run_scoped(forward, VMEM((N, FF), bf16), SEM)

    def backward(ACC, *sums):
        go.sums(ACC, *sums)
        dy_in.wait()

        def last_layer(acc, stg, ss, sd):
            B, nt = T2 // S2, N // T2

            def leave(it):
                return local(stg.at[it % 2], dgus.at[times(it % nt, T2), times(it // nt, WIDE)], ss.at[it % 2])

            def leave_down(j):
                return local(acc.at[j % 2], dws.at[1, j], sd.at[j % 2])

            def tile(it):
                j, t, slot, here = it // nt, it % nt, it % 2, it // nt % 2
                r = times(t, T2)
                again(it, leave(it))
                pl.when((t == 0) & (j >= 2))(leave_down(j).wait)
                go.step2(j, t)
                w, wdn = WGU[1, :, times(j, WIDE)], WD[1, times(j, C), :]
                dgu, p = [], []
                for k in range(S2):
                    rr = pl.ds(t * T2 + k * B, B)
                    gu = dot(A[rr, :], w)
                    by_gu, hidden = back(gu[:, :C], gu[:, C:], dot(DY[rr, :], wdn, NT))
                    stg[slot, pl.ds(k * B, B)] = by_gu
                    dgu.append(by_gu)
                    p.append(hidden.astype(bf16))
                ACC[...] = added(t, ACC[...], dot(A[r, :], jnp.concatenate(dgu), TN))
                acc[here] = added(t, acc[here], dot(jnp.concatenate(p), DY[r, :], TN))
                leave(it).start()

                @pl.when(t == nt - 1)
                def _():
                    leave_down(j).start()
                    go.end2(j)

            loop(NC * nt, tile)
            arrive(map(leave, range(2)))
            arrive(map(leave_down, range(2)))

        pl.run_scoped(last_layer, VMEM((2, C, D), f32), VMEM((2, T2, WIDE), bf16), PAIR, PAIR)

        def first_layer(acc, part, sd, sl):
            go.downs(part, sl)

            def between(sg, sp, sh, *sems):
                B, M, nt = T3 // S3, FF // M3, N // T3

                def come(t):
                    pairs = (dgus, sg), (ps, sp), (h1s, sh)
                    return [local(src.at[times(t, T3)], dst.at[t % 2], sem.at[t % 2]) for (src, dst), sem in zip(pairs, sems)]

                def tile(t):
                    slot = t % 2
                    fetch(t, nt, come)
                    pl.when(t == 0)(a_in.start)
                    arrive(come(t))
                    dh = []
                    for k in range(S3):
                        rr = pl.ds(t * T3 + k * B, B)
                        da = dot(sg[slot, pl.ds(k * B, B), :], WGU[1], NT)
                        dh.append(norm_back(sh[slot, pl.ds(k * B, B)], da, DY[rr, :]))
                        DY[rr, :] = dh[-1]
                    dh = jnp.concatenate(dh)
                    for m in range(M3):
                        c = pl.ds(m * M, M)
                        acc[c, :] = added(t, acc[c, :], dot(sp[slot, :, c], dh, TN))
                    go.step3(t)

                loop(nt, tile)

            pl.run_scoped(between, VMEM((2, T3, BOTH), bf16), VMEM((2, T3, FF), bf16), VMEM((2, T3, D), bf16), PAIR, PAIR, PAIR)
            for s in range(NC):
                local(acc.at[pl.ds(s * C, C)], dws.at[0, s], sd).start()

            def chunks(stg, sin, ss, si):
                B, nt = T4 // S4, N // T4

                def come(it):
                    return [local(gus.at[it // nt, times(it % nt, T4)], sin.at[it % 2], si.at[it % 2])]

                def leave(it):
                    return local(stg.at[it % 2], dgus.at[times(it % nt, T4), times(it // nt, WIDE)], ss.at[it % 2])

                def tile(it):
                    j, t, slot = it // nt, it % nt, it % 2
                    fetch(it, NC * nt, come)
                    again(it, leave(it))
                    go.step4(it)
                    arrive(come(it))
                    wdn = WD[0, times(j, C), :]
                    dgu = []
                    for k in range(S4):
                        dp = dot(DY[pl.ds(t * T4 + k * B, B), :], wdn, NT)
                        gu = sin[slot, pl.ds(k * B, B), :]
                        by_gu, _ = back(gu[:, :C], gu[:, C:], dp)
                        stg[slot, pl.ds(k * B, B)] = by_gu
                        dgu.append(by_gu)
                    ACC[...] = added(t, ACC[...], dot(A[times(t, T4), :], jnp.concatenate(dgu), TN))
                    leave(it).start()

                loop(NC * nt, tile)
                arrive(map(leave, range(2)))

            go.before4(acc, sd)
            a_in.wait()
            pl.run_scoped(chunks, VMEM((2, T4, WIDE), bf16), VMEM((2, T4, WIDE), f32), PAIR, PAIR)

        pl.run_scoped(first_layer, VMEM((FF, D), f32), VMEM((NC, PIECE, D), f32), SEM, SEM)

        def last(sg, sh, so, ss, *sems):
            B, nt = T5 // S5, N // T5

            def come(t):
                pairs = (dgus, sg), (x, sh)
                return [local(src.at[times(t, T5)], dst.at[t % 2], sem.at[t % 2]) for (src, dst), sem in zip(pairs, sems)]

            def leave(t):
                return local(so.at[t % 2], dx.at[times(t, T5)], ss.at[t % 2])

            def tile(t):
                slot = t % 2
                fetch(t, nt, come)
                again(t, leave(t))
                go.step5(t)
                arrive(come(t))
                for k in range(S5):
                    da = dot(sg[slot, pl.ds(k * B, B), :], WGU[0], NT)
                    so[slot, pl.ds(k * B, B)] = norm_back(sh[slot, pl.ds(k * B, B)], da, DY[pl.ds(t * T5 + k * B, B), :])
                leave(t).start()

            loop(nt, tile)
            arrive(map(leave, range(2)))

        pl.run_scoped(last, VMEM((2, T5, BOTH), bf16), VMEM((2, T5, D), bf16), VMEM((2, T5, D), bf16), PAIR, PAIR, PAIR)
        go.close()

    pl.run_scoped(backward, VMEM((D, WIDE), f32), *go.scratch())


class Links:
    def __init__(self, wg, wu, wd, og, od, dws, WGU, WD, CR, XR, ZR, wsem, csem, xsem, zsem, osem, cred):
        self.wg, self.wu, self.wd, self.og, self.od, self.dws, self.WGU, self.WD = wg, wu, wd, og, od, dws, WGU, WD
        self.CR, self.XR, self.ZR = CR, XR, ZR
        self.wsem, self.csem, self.xsem, self.zsem, self.osem, self.cred = wsem, csem, xsem, zsem, osem, cred
        s = lax.axis_index("s")
        self.z, self.s = lax.axis_index("r"), s
        x, y, c = s // 4, (s // 2) % 2, s % 2
        self.c, self.chip = c, s // 2

        def at(x, y, c):
            return 4 * x + 2 * y + c

        self.partner, self.xn, self.yn, self.dn = at(x, y, 1 - c), at(1 - x, y, c), at(x, 1 - y, c), at(1 - x, 1 - y, c)
        self.planes = (self.xn, self.yn, self.dn)

    def to(self, s=None, z=None):
        return (0, self.z if z is None else z, self.s if s is None else s)

    def beyond(self, k):
        return lax.rem(self.z + k, 4)

    def remote(self, src, dst, send, recv, to):
        copy = pltpu.make_async_remote_copy(src, dst, send, recv, device_id=to, device_id_type=MESH)
        copy.start()


    def where(self, u):
        layer, v = u // PER, u % PER
        if layer == 0:
            return layer, v < 8, v if v < 8 else v - 8
        return layer, v == 0 or v >= 5, 0 if v == 0 else (v - 1 if v < 5 else v - 4)

    def piece(self, u, s, half=None):
        layer, gate, k = self.where(u)
        size = ROWS if gate else PIECE
        start, size = (0, size) if half is None else (half * size // 2, size // 2)
        if gate:
            return self.WGU.at[layer, pl.ds(pl.multiple_of(s * ROWS + start, 16), size), pl.ds(k * WIDE, WIDE)]
        return self.WD.at[layer, pl.ds(pl.multiple_of(s * C + k * PIECE + start, 16), size), :]

    def took(self, u, sem, pieces):
        layer, gate, k = self.where(u)
        ref = self.WGU.at[layer, pl.ds(0, ROWS * pieces), pl.ds(0, WIDE)] if gate else self.WD.at[layer, pl.ds(0, PIECE * pieces), :]
        local(ref, ref, sem).wait()

    def own(self, u):
        layer, gate, k = self.where(u)
        sem = self.wsem.at[0, u]
        if gate:
            rows = pl.ds(pl.multiple_of(self.s * ROWS, 16), ROWS)
            local(self.wg.at[layer, :, pl.ds(k * C, C)], self.WGU.at[layer, rows, pl.ds(k * WIDE, C)], sem).start()
            local(self.wu.at[layer, :, pl.ds(k * C, C)], self.WGU.at[layer, rows, pl.ds(k * WIDE + C, C)], sem).start()
        else:
            local(self.wd.at[layer, pl.ds(k * PIECE, PIECE), :], self.piece(u, self.s), sem).start()

    def first(self, u):
        self.took(u, self.wsem.at[0, u], 1)
        mine = self.piece(u, self.s)
        for to, sem in ((self.xn, 2), (self.yn, 2), (self.partner, 4)):
            self.remote(mine, mine, self.wsem.at[1, u], self.wsem.at[sem, u], self.to(to))

    def second(self, u):
        self.took(u, self.wsem.at[2, u], 2)
        for source, half, to in ((self.xn, 0, self.yn), (self.yn, 1, self.xn)):
            ref = self.piece(u, source, half)
            self.remote(ref, ref, self.wsem.at[1, u], self.wsem.at[3, u], self.to(to))
        for source in (self.xn, self.yn):
            ref = self.piece(u, source)
            self.remote(ref, ref, self.wsem.at[1, u], self.wsem.at[4, u], self.to(self.partner))

    def third(self, u):
        self.took(u, self.wsem.at[3, u], 1)
        ref = self.piece(u, self.dn)
        self.remote(ref, ref, self.wsem.at[1, u], self.wsem.at[4, u], self.to(self.partner))

    def whole(self, u):
        self.took(u, self.wsem.at[4, u], 4)

    def pass_on(self, it):
        for u in range(2, LAST):
            if (5 * u - 6) // 3 == it:
                self.second(u)
                self.first(u + 2)
        for u in range(1, LAST):
            if 5 * u // 3 == it:
                self.third(u)

    def open(self):
        self.own(0)
        self.own(1)
        barrier = pltpu.get_barrier_semaphore()
        peers = [self.to(self.partner)] + [self.to(s) for s in self.planes] + [self.to(z=self.beyond(k)) for k in OTHERS]
        for peer in peers:
            pl.semaphore_signal(barrier, inc=1, device_id=peer, device_id_type=MESH)
        pl.semaphore_wait(barrier, len(peers))
        self.first(0)
        self.first(1)
        for u in range(2, UNITS):
            self.own(u)

    def weights_first(self):
        self.second(0)
        self.first(2)
        self.second(1)
        self.first(3)
        self.third(0)

    def step0(self, it):
        for k in range(2 * NC):
            @pl.when(it == k)
            def _():
                self.pass_on(k)
                if k % 2 == 0:
                    self.whole(k // 2)

    def step1(self, t):
        @pl.when(t == 0)
        def _():
            for it in (2 * NC, 2 * NC + 1):
                self.pass_on(it)
            for u in range(NC, PER):
                if 5 * u // 3 >= 2 * NC + 2:
                    self.third(u)
            for u in range(NC, PER):
                self.whole(u)

        for k in range(NC):
            @pl.when(t == k)
            def _():
                for u in range(PER, LAST):
                    if (5 * u - 6) // 3 == k + 2 * NC + 2:
                        self.second(u)
                        self.first(u + 2)
                    if 5 * u // 3 == k + 2 * NC + 2:
                        self.third(u)


    @staticmethod
    def scratch():
        V = VMEM
        return (
            V((2, 4, ROWS, WIDE), bf16),
            V((2, 4, ROWS, WIDE), f32),
            V((4, 3, ROWS, WIDE), bf16),
            V((6, ROWS, WIDE), f32),
            V((4, ROWS, QUARTER), f32),
            V((4, 3, ROWS, QUARTER), bf16),
            V((4, ROWS, QUARTER), f32),
            V((4, ROWS, QUARTER), bf16),
        )

    def sums(self, ACC, CS, OWN, XS, O2, O3, ZS, ZO, F):
        self.ACC, self.CS, self.OWN, self.XS, self.O2, self.O3, self.ZS, self.ZO, self.F = ACC, CS, OWN, XS, O2, O3, ZS, ZO, F

    def done(self, ref, sem):
        local(ref, ref, sem).wait()

    def pack(self, n, block):
        b = n % 2

        @pl.when(n >= 2)
        def _():
            self.done(self.CS.at[b], self.csem.at[0, b])

        for chip in range(4):
            self.CS[b, chip] = block(2 * chip + 1 - self.c).astype(bf16)
            self.OWN[b, chip] = block(2 * chip + self.c)

        @pl.when(n >= 2)
        def _():
            pl.semaphore_wait(self.cred.at[0], 1)

        self.remote(self.CS.at[b], self.CR.at[b], self.csem.at[0, b], self.csem.at[1, b], self.to(self.partner))

    def pack_gate(self, n):
        self.pack(n, lambda s: self.ACC[pl.ds(pl.multiple_of(s * ROWS, 8), ROWS), :])

    def downs(self, part, sem):
        self.part, self.part_sem = part, sem
        self.load_down(1, 0)

    def load_down(self, layer, k):
        local(self.dws.at[layer, :, pl.ds(pl.multiple_of(k * PIECE, 8), PIECE), :], self.part, self.part_sem).start()

    def pack_down(self, n, layer, k):
        self.done(self.part, self.part_sem)

        def block(s):
            rows = []
            for b in range(3):
                cols = slice(b * C, (b + 1) * C)
                rows.append(jnp.concatenate([self.part[s, 0:HALF, cols], self.part[s, HALF:PIECE, cols]], 1))
            return jnp.concatenate(rows, 0)

        self.pack(n, block)

        @pl.when(k < 3)
        def _():
            self.load_down(layer, k + 1)

    def plane(self, n):
        b, xs, xb = n % 2, n % 4, n % 6

        @pl.when(n >= 4)
        def _():
            self.done(self.XS.at[xs], self.xsem.at[0, xs])

        self.done(self.CR.at[b], self.csem.at[1, b])

        def total(chip):
            return self.OWN[b, chip] + self.CR[b, chip].astype(f32)

        for m, s in enumerate(self.planes):
            self.XS[xs, m] = total(s // 2).astype(bf16)
        self.O2[xb] = total(self.chip)

        @pl.when(n + 2 < UNITS)
        def _():
            pl.semaphore_signal(self.cred.at[0], inc=1, device_id=self.to(self.partner), device_id_type=MESH)

        @pl.when(n >= 6)
        def _():
            for m in range(3):
                pl.semaphore_wait(self.cred.at[1 + m], 1)

        for m, s in enumerate(self.planes):
            self.remote(self.XS.at[xs, m], self.XR.at[xb, m], self.xsem.at[0, xs], self.xsem.at[1, xb], self.to(s))

    def line(self, n):
        xb, zb = n % 6, n % 4

        @pl.when(n >= 4)
        def _():
            self.done(self.ZS.at[zb], self.zsem.at[0, zb])

        self.done(self.XR.at[xb], self.xsem.at[1, xb])
        total = self.O2[xb] + self.XR[xb, 0].astype(f32) + self.XR[xb, 1].astype(f32) + self.XR[xb, 2].astype(f32)
        for q in range(4):
            self.O3[q] = total[:, q * QUARTER : (q + 1) * QUARTER]
        self.ZO[zb] = self.O3[self.z]
        for k in OTHERS:
            self.ZS[zb, k - 1] = self.O3[self.beyond(k)].astype(bf16)

        @pl.when(n + 6 < UNITS)
        def _():
            for m, s in enumerate(self.planes):
                pl.semaphore_signal(self.cred.at[1 + m], inc=1, device_id=self.to(s), device_id_type=MESH)

        @pl.when(n >= 4)
        def _():
            for k in OTHERS:
                pl.semaphore_wait(self.cred.at[3 + k], 1)

        for k in OTHERS:
            self.remote(self.ZS.at[zb, k - 1], self.ZR.at[zb, 3 - k], self.zsem.at[0, zb], self.zsem.at[1, zb], self.to(z=self.beyond(k)))

    def final(self, n):
        zb = n % 4

        @pl.when(n >= 4)
        def _():
            self.sent_final(zb)

        self.done(self.ZR.at[zb], self.zsem.at[1, zb])
        total = self.ZO[zb] + self.ZR[zb, 0].astype(f32) + self.ZR[zb, 1].astype(f32) + self.ZR[zb, 2].astype(f32)
        self.F[zb] = total.astype(bf16)

        @pl.when(n + 4 < UNITS)
        def _():
            for k in OTHERS:
                pl.semaphore_signal(self.cred.at[3 + 4 - k], inc=1, device_id=self.to(z=self.beyond(k)), device_id_type=MESH)

        own, other = self.osem.at[1, zb], self.osem.at[0, zb]
        half = self.z // 2
        layer = 1 - n // PER

        def gate(j):
            place = self.og.at[half, layer, :, pl.ds(pl.multiple_of(j * C + self.z % 2 * QUARTER, QUARTER), QUARTER)]
            local(self.F.at[zb], place, own).start()
            for k in OTHERS:
                self.remote(self.F.at[zb], place, other, self.osem.at[2, 0], self.to(z=self.beyond(k)))

        def down(k):
            for b in range(3):
                src = self.F.at[zb, pl.ds(b * HALF, HALF)]
                place = self.od.at[layer, pl.ds(pl.multiple_of(k * PIECE + half * HALF, HALF), HALF), pl.ds(pl.multiple_of(b * C + self.z % 2 * QUARTER, QUARTER), QUARTER)]
                local(src, place, own).start()
                for k_ in OTHERS:
                    self.remote(src, place, other, self.osem.at[2, 1], self.to(z=self.beyond(k_)))

        early = (n >= PER) & (n < 20)
        pl.when((n < 8) | (n >= 20))(lambda: gate(n - 16 * (n // PER)))
        pl.when(early & (n % 2 == 1))(lambda: gate((n - 13) // 2))
        pl.when((n >= 8) & (n < PER))(lambda: down(n - 8))
        pl.when(early & (n % 2 == 0))(lambda: down((n - PER) // 2))

    def sent_final(self, zb):
        self.done(self.F.at[zb], self.osem.at[1, zb])
        ref = self.ZR.at[zb]
        local(ref, ref, self.osem.at[0, zb]).wait()

    def step2(self, j, t):
        for k in range(NC):
            @pl.when((t == 0) & (j == k))
            def _():
                if k == 0:
                    self.third(LAST - 1)
                for u in range(PER if k == 0 else LAST - 1 + k, LAST + k):
                    self.whole(u)
                if LAST + k < UNITS:
                    self.second(LAST + k)
                if LAST + 2 + k < UNITS:
                    self.first(LAST + 2 + k)

            if LAST + k < UNITS:
                @pl.when((t == 1) & (j == k))
                def _():
                    self.third(LAST + k)

        for back, stage in ((3, self.final), (2, self.line), (1, self.plane)):
            @pl.when((t == 1) & (j >= back))
            def _():
                stage(j - back)

    def end2(self, j):
        self.pack_gate(j)

    def step3(self, t):
        for back, stage, last in ((3, self.final, 6), (2, self.line, 5), (1, self.plane, 4)):
            @pl.when(t <= last)
            def _():
                stage(8 + t - back)

        @pl.when(t <= 3)
        def _():
            self.pack_down(8 + t, 1, t)

    def before4(self, acc_d, sem):
        self.acc_d, self.acc_sem = acc_d, sem

    def step4(self, it):
        @pl.when(it == 0)
        def _():
            self.done(self.acc_d, self.acc_sem)
            self.load_down(0, 0)

        for start, stage in ((7, self.final), (5, self.line)):
            @pl.when((it >= start) & ((it - start) % 3 != 1))
            def _():
                stage(PER + (2 * (it - start) + 1) // 3)

        @pl.when((it >= 2) & (it <= 9))
        def _():
            self.plane(PER + it - 2)

        @pl.when((it >= 11) & (it % 2 == 1))
        def _():
            self.plane(20 + (it - 11) // 2)

        @pl.when((it <= 7) & (it % 2 == 1))
        def _():
            self.pack_down(PER + it - 1, 0, (it - 1) // 2)

        @pl.when((it >= 2) & (it <= 8) & (it % 2 == 0))
        def _():
            self.pack_gate(PER + it - 1)

        @pl.when((it >= 10) & (it % 2 == 0))
        def _():
            self.pack_gate(PER + it // 2 + 3)

    def step5(self, t):
        @pl.when((t >= 1) & (t <= 6))
        def _():
            self.final(17 + t)

        @pl.when(t <= 4)
        def _():
            self.line(19 + t)

        @pl.when(t == 1)
        def _():
            self.plane(23)

        @pl.when(t == 0)
        def _():
            self.pack_gate(23)

    def close(self):
        for b in range(2):
            self.done(self.CS.at[b], self.csem.at[0, b])
        for b in range(4):
            self.done(self.XS.at[b], self.xsem.at[0, b])
            self.done(self.ZS.at[b], self.zsem.at[0, b])
            self.sent_final(b)
        for u in range(UNITS):
            self.took(u, self.wsem.at[1, u], 7)
        self.done(self.og.at[:, :, :, pl.ds(0, 3 * FF // 4)], self.osem.at[2, 0])
        self.done(self.od.at[:, pl.ds(0, 3 * C // 4)], self.osem.at[2, 1])


def whole(x, dy, wg, wu, wd, dx, og, od, gus, ps, dgus, h1s, a0s, dws, A, DY, WGU, WD, CR, XR, ZR, lsem, wsem, csem, xsem, zsem, osem, cred):
    links = Links(wg, wu, wd, og, od, dws, WGU, WD, CR, XR, ZR, wsem, csem, xsem, zsem, osem, cred)
    kernel(x, dy, wg, wu, wd, dx, og, od, gus, ps, dgus, h1s, a0s, dws, A, DY, WGU, WD, lsem, links)


def solution(mesh):
    def call(x, dy, wg, wu, wd):
        anywhere = pl.BlockSpec(memory_space=pl.ANY)
        S, V, M = jax.ShapeDtypeStruct, VMEM, SEM
        flops = 17 * 2 * N * D * FF
        out = pl.pallas_call(
            whole,
            in_specs=[anywhere] * 5,
            out_specs=[anywhere] * 9,
            out_shape=[
                S((N, D), bf16),
                S((2, 2, ROWS, FF), bf16),
                S((2, C, D), bf16),
                S((NC, N, WIDE), f32),
                S((N, FF), bf16),
                S((N, BOTH), bf16),
                S((N, D), bf16),
                S((N, D), bf16),
                S((2, 8, C, D), f32),
            ],
            scratch_shapes=[
                V((N, D), bf16),
                V((N, D), bf16),
                V((2, D, BOTH), bf16),
                V((2, FF, D), bf16),
                V((2, 4, ROWS, WIDE), bf16),
                V((6, 3, ROWS, WIDE), bf16),
                V((4, 3, ROWS, QUARTER), bf16),
                M((2,)),
                M((5, UNITS)),
                M((2, 2)),
                M((2, 6)),
                M((2, 4)),
                M((3, 4)),
                pltpu.SemaphoreType.REGULAR((7,)),
            ],
            compiler_params=pltpu.CompilerParams(vmem_limit_bytes=67_000_000, collective_id=0, has_side_effects=True),
            cost_estimate=pl.CostEstimate(flops=flops, bytes_accessed=400_000_000, transcendentals=0),
            name="stack",
        )(x, dy, wg, wu, wd)
        return out[:3]

    def step(x, dy, wg, wu, wd):
        dx, gates, downs = call(x[0], dy[0], wg, wu, wd)
        return dx[None], gates[0], gates[1], downs

    states, cut = P(("rep", "r", "s"), None, None), P(None, "s", None)
    return jax.shard_map(
        step,
        mesh=mesh,
        in_specs=(states, states) + (cut,) * 3,
        out_specs=(states,) + (P("rep", "s", None),) * 3,
        check_vma=False,
    )
```

```python
import functools

import jax
import jax.numpy as jnp
from jax import lax
from jax.experimental import pallas as pl
from jax.experimental.pallas import tpu as pltpu
from jax.sharding import PartitionSpec as P

N, D, FF = 4096, 768, 2048
C, NC = 256, 8
WIDE, BOTH = 2 * C, 2 * FF
QUARTER, PIECE, HALF = C // 2, C // 4, C // 8
ROWS = D // NC
UNITS = 24
PER = UNITS // 2
DOWNS = (NC, PER + 1)
LAST = 17
OTHERS = (1, 2, 3)
T0, T1, T2, T3, T4, T5 = FF, WIDE, FF, WIDE, FF, WIDE
S0, S1, S2, S3, S4, S5 = 4, 2, 4, 2, 4, 2
M3 = 4
f32, bf16 = jnp.float32, jnp.bfloat16
NN = (((1,), (0,)), ((), ()))
NT = (((1,), (1,)), ((), ()))
TN = (((0,), (0,)), ((), ()))
MESH = pl.DeviceIdType.MESH
VMEM, SEM = pltpu.VMEM, pltpu.SemaphoreType.DMA
PAIR = SEM((2,))
local = pltpu.make_async_copy


def dot(a, b, dims=NN):
    return lax.dot_general(a, b, dims, preferred_element_type=f32)


def scale_of(wide):
    return lax.rsqrt(jnp.mean(wide * wide, -1, keepdims=True) + 1e-6)


def normed(h):
    wide = h.astype(f32)
    return (wide * scale_of(wide)).astype(bf16)


def norm_back(h, by_a, by_out):
    wide = h.astype(f32)
    by_a = by_a.astype(bf16).astype(f32)
    scale = scale_of(wide)
    along = jnp.mean(by_a * wide, -1, keepdims=True) * (scale * scale * scale)
    return (by_out.astype(f32) + (by_a * scale - wide * along).astype(bf16).astype(f32)).astype(bf16)


def back(g, u, dp):
    dp = dp.astype(bf16).astype(f32)
    s = jax.nn.sigmoid(g)
    sg = g * s
    return jnp.concatenate([(dp * u * (s + sg * (1 - s))).astype(bf16), (dp * sg).astype(bf16)], 1), sg * u


def times(start, size):
    return pl.ds(pl.multiple_of(start * size, size), size)


def loop(count, body):
    def step(i, carry):
        body(i)
        return carry

    lax.fori_loop(0, count, step, 0)


def fetch(i, count, copies, started=False):
    @pl.when((i == 0) & (not started))
    def _():
        for c in copies(i):
            c.start()

    @pl.when(i + 1 < count)
    def _():
        for c in copies(i + 1):
            c.start()


def arrive(copies):
    for c in copies:
        c.wait()


def again(i, copy):
    pl.when(i >= 2)(copy.wait)


def gates(ref, layer, cols=slice(None)):
    w = ref[layer, :, :, :, cols]
    return w.reshape(D, w.shape[-1])


def choose(i, cases, low=0):
    if len(cases) == 1:
        return cases[0]()
    half = len(cases) // 2
    pl.when(i < low + half)(lambda: choose(i, cases[:half], low))
    pl.when(i >= low + half)(lambda: choose(i, cases[half:], low + half))


def added(t, ref, term):
    return jnp.where(t == 0, 0.0, ref) + term


def kernel(x, dy, wg, wu, wd, dx, og, od, gus, ps, dgus, h1s, a0s, dws, A, DY, WGU, WD, lsem, go):
    x_in, dy_in = local(x, A, lsem.at[0]), local(dy, DY, lsem.at[1])
    a_out, a_in = local(A, a0s, lsem.at[0]), local(a0s, A, lsem.at[0])
    x_in.start()
    dy_in.start()
    go.open()
    x_in.wait()

    @functools.partial(loop, N // C)
    def _(t):
        A[times(t, C), :] = normed(A[times(t, C), :])

    a_out.start()
    go.weights_first()

    def forward(hid, stg, stx, sth, sp, ss, sx, sh):
        x_tile = states_in(stx, sx)
        arrive_later = x_tile(0)
        for c in arrive_later:
            c.start()
        kept = hidden0(hid, stg, ss)
        a_out.wait()
        local(hid, ps, sp).start()
        states1(hid, stx, sth, x_tile, sh)
        arrive(kept)
        local(hid, ps, sp).wait()

    def states_in(stx, sx):
        return lambda t: [local(x.at[times(t, T1)], stx.at[t % 2], sx.at[t % 2])]

    def hidden0(hid, stg, ss):
        B, nt = T0 // S0, N // T0

        def leave(it):
            return local(stg.at[it % 2], gus.at[it // nt, times(it % nt, T0)], ss.at[it % 2])

        def tile(it):
            j, t, slot = it // nt, it % nt, it % 2
            again(it, leave(it))
            go.step0(it)
            w = gates(WGU, 0, times(j, WIDE))
            for k in range(S0):
                gu = dot(A[pl.ds(t * T0 + k * B, B), :], w)
                stg[slot, pl.ds(k * B, B)] = gu
                g, u = gu[:, :C], gu[:, C:]
                hid[pl.ds(t * T0 + k * B, B), times(j, C)] = (g * jax.nn.sigmoid(g) * u).astype(bf16)
            leave(it).start()

        loop(NC * nt, tile)
        return map(leave, range(2))

    def states1(hid, stx, sth, come, ss):
        B, nt = T1 // S1, N // T1

        def leave(t):
            return local(sth.at[t % 2], h1s.at[times(t, T1)], ss.at[t % 2])

        def tile(t):
            slot = t % 2
            fetch(t, nt, come, True)
            again(t, leave(t))
            arrive(come(t))
            go.step1(t)
            for k in range(S1):
                m = dot(hid[pl.ds(t * T1 + k * B, B), :], WD[0].reshape(FF, D)).astype(bf16)
                h = (stx[slot, pl.ds(k * B, B)].astype(f32) + m.astype(f32)).astype(bf16)
                sth[slot, pl.ds(k * B, B)] = h
                A[pl.ds(t * T1 + k * B, B), :] = normed(h)
            leave(t).start()

        loop(nt, tile)
        arrive(map(leave, range(2)))

    tiles1 = VMEM((2, T1, D), bf16)
    pl.run_scoped(forward, VMEM((N, FF), bf16), VMEM((2, T0, WIDE), f32), tiles1, tiles1, SEM, PAIR, PAIR, PAIR)

    def backward(ACC, *sums):
        go.sums(ACC, *sums)
        dy_in.wait()

        def last_layer(acc, stg, ss, sd):
            B, nt = T2 // S2, N // T2

            def leave(it):
                return local(stg.at[it % 2], dgus.at[times(it % nt, T2), times(it // nt, WIDE)], ss.at[it % 2])

            def leave_down(j):
                return local(acc.at[j % 2], dws.at[j], sd.at[j % 2])

            def tile(it):
                j, t, slot, here = it // nt, it % nt, it % 2, it // nt % 2
                r = times(t, T2)
                again(it, leave(it))
                pl.when((t == 0) & (j >= 2))(leave_down(j).wait)
                go.step2(j, t)
                w, wdn = gates(WGU, 1, times(j, WIDE)), WD[1, j // 2, j % 2]
                dgu, p = [], []
                for k in range(S2):
                    rr = pl.ds(t * T2 + k * B, B)
                    gu = dot(A[rr, :], w)
                    by_gu, hidden = back(gu[:, :C], gu[:, C:], dot(DY[rr, :], wdn, NT))
                    stg[slot, pl.ds(k * B, B)] = by_gu
                    dgu.append(by_gu)
                    p.append(hidden.astype(bf16))
                ACC[...] = added(t, ACC[...], dot(A[r, :], jnp.concatenate(dgu), TN).reshape(ACC.shape))
                acc[here] = added(t, acc[here], dot(jnp.concatenate(p), DY[r, :], TN))
                leave(it).start()

                @pl.when(t == nt - 1)
                def _():
                    leave_down(j).start()
                    go.end2(j)

            loop(NC * nt, tile)
            arrive(map(leave, range(2)))
            arrive(map(leave_down, range(2)))

        pl.run_scoped(last_layer, VMEM((2, C, D), f32), VMEM((2, T2, WIDE), bf16), PAIR, PAIR)

        def first_layer(acc, sl):
            go.downs(acc, sl)

            def between(sg, sp, sh, *sems):
                B, M, nt = T3 // S3, FF // M3, N // T3

                def come(t):
                    pairs = (dgus, sg), (ps, sp), (h1s, sh)
                    return [local(src.at[times(t, T3)], dst.at[t % 2], sem.at[t % 2]) for (src, dst), sem in zip(pairs, sems)]

                def tile(t):
                    slot = t % 2
                    fetch(t, nt, come)
                    pl.when(t == 0)(a_in.start)
                    arrive(come(t))
                    dh = []
                    for k in range(S3):
                        rr = pl.ds(t * T3 + k * B, B)
                        da = dot(sg[slot, pl.ds(k * B, B), :], gates(WGU, 1), NT)
                        dh.append(norm_back(sh[slot, pl.ds(k * B, B)], da, DY[rr, :]))
                        DY[rr, :] = dh[-1]
                    dh = jnp.concatenate(dh)
                    for m in range(M3):
                        c = pl.ds(m * M, M)
                        acc[c, :] = added(t, acc[c, :], dot(sp[slot, :, c], dh, TN))
                    go.step3(t)

                loop(nt, tile)

            pl.run_scoped(between, VMEM((2, T3, BOTH), bf16), VMEM((2, T3, FF), bf16), VMEM((2, T3, D), bf16), PAIR, PAIR, PAIR)

            def chunks(stg, sin, ss, si):
                B, nt = T4 // S4, N // T4

                def come(it):
                    return [local(gus.at[it // nt, times(it % nt, T4)], sin.at[it % 2], si.at[it % 2])]

                def leave(it):
                    return local(stg.at[it % 2], dgus.at[times(it % nt, T4), times(it // nt, WIDE)], ss.at[it % 2])

                def tile(it):
                    j, t, slot = it // nt, it % nt, it % 2
                    fetch(it, NC * nt, come)
                    again(it, leave(it))
                    go.step4(it)
                    arrive(come(it))
                    wdn = WD[0, j // 2, j % 2]
                    dgu = []
                    for k in range(S4):
                        dp = dot(DY[pl.ds(t * T4 + k * B, B), :], wdn, NT)
                        gu = sin[slot, pl.ds(k * B, B), :]
                        by_gu, _ = back(gu[:, :C], gu[:, C:], dp)
                        stg[slot, pl.ds(k * B, B)] = by_gu
                        dgu.append(by_gu)
                    ACC[...] = added(t, ACC[...], dot(A[times(t, T4), :], jnp.concatenate(dgu), TN).reshape(ACC.shape))
                    leave(it).start()

                loop(NC * nt, tile)
                arrive(map(leave, range(2)))

            a_in.wait()
            pl.run_scoped(chunks, VMEM((2, T4, WIDE), bf16), VMEM((2, T4, WIDE), f32), PAIR, PAIR)

        pl.run_scoped(first_layer, VMEM((FF, D), f32), SEM)

        def last(sg, sh, so, ss, *sems):
            B, nt = T5 // S5, N // T5

            def come(t):
                pairs = (dgus, sg), (x, sh)
                return [local(src.at[times(t, T5)], dst.at[t % 2], sem.at[t % 2]) for (src, dst), sem in zip(pairs, sems)]

            def leave(t):
                return local(so.at[t % 2], dx.at[times(t, T5)], ss.at[t % 2])

            def tile(t):
                slot = t % 2
                fetch(t, nt, come)
                again(t, leave(t))
                go.step5(t)
                arrive(come(t))
                for k in range(S5):
                    da = dot(sg[slot, pl.ds(k * B, B), :], gates(WGU, 0), NT)
                    so[slot, pl.ds(k * B, B)] = norm_back(sh[slot, pl.ds(k * B, B)], da, DY[pl.ds(t * T5 + k * B, B), :])
                leave(t).start()

            loop(nt, tile)
            arrive(map(leave, range(2)))

        pl.run_scoped(last, VMEM((2, T5, BOTH), bf16), VMEM((2, T5, D), bf16), VMEM((2, T5, D), bf16), PAIR, PAIR, PAIR)
        go.close()

    pl.run_scoped(backward, VMEM((NC, ROWS, WIDE), f32), *go.scratch())


class Links:
    def __init__(self, wg, wu, wd, og, od, dws, WGU, WD, CR, XR, ZR, wsem, csem, xsem, zsem, osem, cred):
        self.wg, self.wu, self.wd, self.og, self.od, self.dws, self.WGU, self.WD = wg, wu, wd, og, od, dws, WGU, WD
        self.CR, self.XR, self.ZR = CR, XR, ZR
        self.wsem, self.csem, self.xsem, self.zsem, self.osem, self.cred = wsem, csem, xsem, zsem, osem, cred
        s, z = lax.axis_index("s"), lax.axis_index("r")
        self.z, self.s = z, s
        x, y, c = s // 4, s // 2 % 2, s % 2
        self.core, self.chip = c, s // 2
        self.chips = 2 * (1 - x) + y, 2 * x + 1 - y, 2 * (1 - x) + 1 - y
        self.planes = [2 * q + c for q in self.chips]
        self.partner = s + 1 - 2 * c
        self.lines = z + 1 - 2 * (z % 2), (z + 2) % 4

    def to(self, s=None, z=None):
        return (0, self.z if z is None else z, self.s if s is None else s)

    def remote(self, src, dst, send, recv, to):
        pltpu.make_async_remote_copy(src, dst, send, recv, device_id=to, device_id_type=MESH).start()

    def done(self, ref, sem):
        local(ref, ref, sem).wait()


    def kind(self, u):
        if not isinstance(u, int):
            return 1, True, u - LAST + 1
        layer, v = u // PER, u % PER
        if layer == 0:
            return layer, v < NC, v % NC
        return layer, v == 0 or v > 4, v - 4 if v > 4 else max(v - 1, 0)

    def unit(self, u, chip, core, rows=None):
        layer, gate, k = self.kind(u)
        if gate:
            return self.WGU.at[layer, chip, core, rows or slice(None), times(k, WIDE)]
        start, size = (rows.start, rows.size) if rows else (0, PIECE)
        return self.WD.at[layer, chip, core, pl.ds(k * PIECE + start, size), :]

    def own(self, u):
        layer, gate, k = self.kind(u)
        sem = self.wsem.at[0, u]
        if gate:
            for w, side in ((self.wg, 0), (self.wu, C)):
                local(w.at[layer, :, pl.ds(k * C, C)], self.WGU.at[layer, self.chip, self.core, :, pl.ds(k * WIDE + side, C)], sem).start()
        elif k == 0:
            local(self.wd.at[layer], self.WD.at[layer, self.chip, self.core], sem).start()

    def first(self, u):
        layer, gate, k = self.kind(u)
        mine = self.unit(u, self.chip, self.core)
        if gate:
            self.done(mine, self.wsem.at[0, u])
        elif k == 0:
            self.done(self.WD.at[layer, self.chip, self.core], self.wsem.at[0, u])
        for to in self.planes[:2]:
            self.remote(mine, mine, self.wsem.at[1, u], self.wsem.at[2, u], self.to(to))

    def second(self, u):
        self.done(self.unit(u, 0, pl.ds(0, 2)), self.wsem.at[2, u])
        size = (ROWS if self.kind(u)[1] else PIECE) // 2
        for half in range(2):
            ref = self.unit(u, self.chips[half], self.core, pl.ds(half * size, size))
            self.remote(ref, ref, self.wsem.at[1, u], self.wsem.at[3, u], self.to(self.planes[1 - half]))

    def third(self, u):
        self.done(self.unit(u, 0, 0), self.wsem.at[3, u])
        ref = self.unit(u, slice(None), self.core)
        self.remote(ref, ref, self.wsem.at[5, u], self.wsem.at[4, u], self.to(self.partner))

    def whole(self, u):
        self.done(self.unit(u, slice(None), 0), self.wsem.at[4, u])

    def pass_on(self, it):
        for u in range(2, LAST):
            if (5 * u - 6) // 3 == it:
                self.second(u)
                self.first(u + 2)
        for u in range(1, LAST):
            if 5 * u // 3 == it:
                self.third(u)

    def open(self):
        self.own(0)
        self.own(1)
        barrier = pltpu.get_barrier_semaphore()
        peers = [self.to(self.partner)] + [self.to(s) for s in self.planes] + [self.to(z=z) for z in self.lines]
        for peer in peers:
            pl.semaphore_signal(barrier, inc=1, device_id=peer, device_id_type=MESH)
        pl.semaphore_wait(barrier, len(peers))
        self.first(0)
        self.first(1)
        for u in range(2, NC + 1):
            self.own(u)

    def weights_first(self):
        self.second(0)
        self.first(2)
        self.second(1)
        self.first(3)
        self.third(0)

    def step0(self, it):
        def case(k):
            self.pass_on(k)
            if k % 2 == 0:
                self.whole(k // 2)
            if PER + k < UNITS:
                self.own(PER + k)

        choose(it, [functools.partial(case, k) for k in range(2 * NC)])

    def step1(self, t):
        def case(k):
            if k == 0:
                self.pass_on(2 * NC)
                self.pass_on(2 * NC + 1)
                for u in range(NC, PER):
                    if 5 * u // 3 >= 2 * NC + 2:
                        self.third(u)
                for u in range(NC, PER):
                    self.whole(u)
            for u in range(PER, LAST):
                if (5 * u - 6) // 3 == k + 2 * NC + 2:
                    self.second(u)
                    self.first(u + 2)
                if 5 * u // 3 == k + 2 * NC + 2:
                    self.third(u)

        choose(t, [functools.partial(case, k) for k in range(NC)])


    @staticmethod
    def scratch():
        blocks, wide = (4, ROWS, WIDE), (ROWS, WIDE)
        return (
            VMEM((2, *blocks), bf16),
            VMEM((2, *blocks), f32),
            VMEM((6, 3, *wide), bf16),
            VMEM((6, *wide), f32),
            VMEM((2, 4, *wide), bf16),
            VMEM((2, *wide), bf16),
            VMEM((2, PIECE, D), bf16),
        )

    def sums(self, ACC, CS, OWN, XS, O2, ZS, F, FD):
        self.ACC, self.CS, self.OWN, self.XS, self.O2, self.ZS, self.F, self.FD = ACC, CS, OWN, XS, O2, ZS, F, FD

    def free(self, k, to):
        pl.semaphore_signal(self.cred.at[k], inc=1, device_id=to, device_id_type=MESH)

    def pack(self, n, block):
        b = n % 2
        for chip in range(4):
            self.CS[b, chip] = block(2 * chip + 1 - self.core).astype(bf16)
            self.OWN[b, chip] = block(2 * chip + self.core)

        @pl.when(n >= 2)
        def _():
            pl.semaphore_wait(self.cred.at[0], 1)

        self.remote(self.CS.at[b], self.CR.at[b], self.csem.at[0, b], self.csem.at[1, b], self.to(self.partner))

    def pack_gate(self, n):
        self.pack(n, lambda s: self.ACC[s])

    def downs(self, acc, sem):
        self.acc, self.acc_sem = acc, sem
        self.load_down(0)

    def load_down(self, k):
        for b in range(3):
            for h in range(2):
                src = self.dws.at[:, pl.ds(pl.multiple_of(k * PIECE + h * HALF, HALF), HALF), pl.ds(b * C, C)]
                local(src, self.ACC.at[:, pl.ds(b * HALF, HALF), pl.ds(h * C, C)], self.acc_sem).start()

    def pack_down1(self, n):
        self.done(self.ACC, self.acc_sem)
        self.pack_gate(n)
        pl.when(n < PER - 1)(lambda: self.load_down(n - NC + 1))

    def pack_down0(self, n):
        k = (n - PER) // 2

        def block(s):
            rows = []
            for b in range(3):
                sides = [self.acc[pl.ds(pl.multiple_of(s * C + k * PIECE + h * HALF, HALF), HALF), pl.ds(b * C, C)] for h in range(2)]
                rows.append(jnp.concatenate(sides, 1))
            return jnp.concatenate(rows)

        self.pack(n, block)

    def plane(self, n):
        b, xb = n % 2, n % 6
        for side, ref in enumerate((self.CS, self.CR)):
            self.done(ref.at[b], self.csem.at[side, b])

        def total(chip):
            return self.OWN[b, chip] + self.CR[b, chip].astype(f32)

        for m, chip in enumerate(self.chips):
            self.XS[xb, m] = total(chip).astype(bf16)
        self.O2[xb] = total(self.chip)
        pl.when(n + 2 < UNITS)(lambda: self.free(0, self.to(self.partner)))

        @pl.when(n >= 6)
        def _():
            for m in OTHERS:
                pl.semaphore_wait(self.cred.at[m], 1)

        for m, s in enumerate(self.planes):
            self.remote(self.XS.at[xb, m], self.XR.at[xb, m], self.xsem.at[0, xb], self.xsem.at[1, xb], self.to(s))

    def line(self, n, k, total):
        zb = n % 4
        self.ZS[k, zb] = total.astype(bf16)

        @pl.when(n >= 4)
        def _():
            pl.semaphore_wait(self.cred.at[4 + k], 1)

        self.remote(self.ZS.at[k, zb], self.ZR.at[k, zb], self.zsem.at[k, 0, zb], self.zsem.at[k, 1, zb], self.to(z=self.lines[k]))

    def line_sum(self, n, k):
        zb = n % 4
        for side, ref in enumerate((self.ZS, self.ZR)):
            self.done(ref.at[k, zb], self.zsem.at[k, side, zb])
        total = self.ZS[k, zb].astype(f32) + self.ZR[k, zb].astype(f32)
        pl.when(n + 4 < UNITS)(lambda: self.free(4 + k, self.to(z=self.lines[k])))
        return total

    def line1(self, n):
        xb = n % 6
        for side, ref in enumerate((self.XS, self.XR)):
            self.done(ref.at[xb], self.xsem.at[side, xb])
        total = self.O2[xb] + (self.XR[xb, 0].astype(f32) + self.XR[xb, 1].astype(f32) + self.XR[xb, 2].astype(f32))

        @pl.when(n + 6 < UNITS)
        def _():
            for m, s in zip(OTHERS, self.planes):
                self.free(m, self.to(s))

        self.line(n, 0, total)

    def line2(self, n):
        self.line(n, 1, self.line_sum(n, 0))

    def finish(self, n):
        total = self.line_sum(n, 1).astype(bf16)
        pl.when(n >= 2)(lambda: self.done(self.F.at[n % 2], self.osem.at[n % 2]))
        return total

    def final_gate(self, n, layer, j):
        b = n % 2
        self.F[b] = self.finish(n)
        for side in range(2):
            place = self.og.at[side, layer, :, times(j, C)]
            local(self.F.at[b, :, pl.ds(side * C, C)], place, self.osem.at[b]).start()

    def final_down(self, n, layer, k):
        b = n % 2
        total = self.finish(n)
        for i in range(3):
            for h in range(2):
                self.FD[b, pl.ds(h * HALF, HALF), pl.ds(i * C, C)] = total[i * HALF : (i + 1) * HALF, h * C : (h + 1) * C]
        local(self.FD.at[b], self.od.at[layer, times(k, PIECE)], self.osem.at[b]).start()

    def final1(self, n):
        self.final_gate(n, 1, n)

    def step2(self, j, t):
        @pl.when(t == 0)
        def _():
            @pl.when(j == 0)
            def _():
                self.third(LAST - 1)
                for u in range(PER, LAST):
                    self.whole(u)

            pl.when(j >= 1)(lambda: self.whole(LAST - 1 + j))
            pl.when(j < UNITS - LAST)(lambda: self.second(LAST + j))
            pl.when(j < UNITS - LAST - 2)(lambda: self.first(LAST + 2 + j))

        @pl.when(t == 1)
        def _():
            pl.when(j < UNITS - LAST)(lambda: self.third(LAST + j))
            for back, stage in enumerate((self.plane, self.line1, self.line2, self.final1), 1):
                pl.when(j >= back)(functools.partial(stage, j - back))

    def end2(self, j):
        self.pack_gate(j)

    def step3(self, t):
        pl.when(t <= 3)(lambda: self.final1(4 + t))
        pl.when(t >= 6)(lambda: self.final_down(2 + t, 1, t - 6))
        pl.when(t <= 2)(lambda: self.line2(5 + t))
        pl.when(t >= 4)(lambda: self.line2(4 + t))
        pl.when(t <= 1)(lambda: self.line1(6 + t))
        pl.when((t >= 3) & (t <= 6))(lambda: self.line1(5 + t))
        pl.when(t <= 4)(lambda: self.plane(7 + t))
        pl.when(t <= 3)(lambda: self.pack_down1(8 + t))

    def step4(self, it):
        pl.when(it <= 1)(lambda: self.final_down(PER - 2 + it, 1, 2 + it))
        pl.when((it == 11) | (it == 14))(lambda: self.final_down(PER + (it - 11) // 3 * 2, 0, (it - 11) // 3))
        pl.when(it == 13)(lambda: self.final_gate(PER + 1, 0, 0))
        for start, stage in ((8, self.line2), (6, self.line1)):
            @pl.when((it >= start) & ((it - start) % 3 != 1))
            def _():
                stage(PER + (2 * (it - start) + 1) // 3)

        pl.when((it >= 2) & (it <= 9))(lambda: self.plane(PER + it - 2))
        pl.when((it >= 11) & (it % 2 == 1))(lambda: self.plane(PER + NC + (it - 11) // 2))
        pl.when((it <= 7) & (it % 2 == 1))(lambda: self.pack_down0(PER + it - 1))
        pl.when((it >= 2) & (it <= 8) & (it % 2 == 0))(lambda: self.pack_gate(PER + it - 1))
        pl.when((it >= 10) & (it % 2 == 0))(lambda: self.pack_gate(PER + 3 + it // 2))

    def step5(self, t):
        pl.when((t == 1) | (t == 3))(lambda: self.final_down(PER + 3 + t, 0, (t + 3) // 2))
        pl.when((t == 0) | (t == 2))(lambda: self.final_gate(PER + 3 + t, 0, t // 2 + 1))
        pl.when(t >= 4)(lambda: self.final_gate(PER + 3 + t, 0, t - 1))
        pl.when(t <= 6)(lambda: self.line2(PER + 5 + t))
        pl.when(t <= 4)(lambda: self.line1(PER + 7 + t))
        pl.when(t == 1)(lambda: self.plane(UNITS - 1))
        pl.when(t == 0)(lambda: self.pack_gate(UNITS - 1))

    def close(self):
        self.final_gate(UNITS - 1, 0, NC - 1)
        for b in range(2):
            self.done(self.F.at[b], self.osem.at[b])
        for u in range(UNITS):
            self.done(self.unit(u, pl.ds(0, 3), 0), self.wsem.at[1, u])
            self.done(self.unit(u, slice(None), 0), self.wsem.at[5, u])


def whole(x, dy, wg, wu, wd, dx, og, od, gus, ps, dgus, h1s, a0s, dws, A, DY, WGU, WD, CR, XR, ZR, lsem, wsem, csem, xsem, zsem, osem, cred):
    links = Links(wg, wu, wd, og, od, dws, WGU, WD, CR, XR, ZR, wsem, csem, xsem, zsem, osem, cred)
    kernel(x, dy, wg, wu, wd, dx, og, od, gus, ps, dgus, h1s, a0s, dws, A, DY, WGU, WD, lsem, links)


def solution(mesh):
    def call(x, dy, wg, wu, wd):
        anywhere = pl.BlockSpec(memory_space=pl.ANY)
        S, V, M = jax.ShapeDtypeStruct, VMEM, SEM
        flops = 17 * 2 * N * D * FF
        out = pl.pallas_call(
            whole,
            in_specs=[anywhere] * 5,
            out_specs=[anywhere] * 9,
            out_shape=[
                S((N, D), bf16),
                S((2, 2, ROWS, FF), bf16),
                S((2, C, D), bf16),
                S((NC, N, WIDE), f32),
                S((N, FF), bf16),
                S((N, BOTH), bf16),
                S((N, D), bf16),
                S((N, D), bf16),
                S((NC, C, D), f32),
            ],
            scratch_shapes=[
                V((N, D), bf16),
                V((N, D), bf16),
                V((2, 4, 2, ROWS, BOTH), bf16),
                V((2, 4, 2, C, D), bf16),
                V((2, 4, ROWS, WIDE), bf16),
                V((6, 3, ROWS, WIDE), bf16),
                V((2, 4, ROWS, WIDE), bf16),
                PAIR,
                M((6, UNITS)),
                M((2, 2)),
                M((2, 6)),
                M((2, 2, 4)),
                PAIR,
                pltpu.SemaphoreType.REGULAR((6,)),
            ],
            compiler_params=pltpu.CompilerParams(vmem_limit_bytes=67_000_000, collective_id=0, has_side_effects=True),
            cost_estimate=pl.CostEstimate(flops=flops, bytes_accessed=400_000_000, transcendentals=0),
            name="stack",
        )(x, dy, wg, wu, wd)
        return out[:3]

    def step(x, dy, wg, wu, wd):
        dx, sides, down = call(x[0], dy[0], wg, wu, wd)
        return dx[None], sides[0], sides[1], down

    states, cut = P(("rep", "r", "s"), None, None), P(None, "s", None)
    return jax.shard_map(
        step,
        mesh=mesh,
        in_specs=(states, states) + (cut,) * 3,
        out_specs=(states,) + (P("rep", "s", None),) * 3,
        check_vma=False,
    )
```

```python
import functools

import jax
import jax.numpy as jnp
from jax import lax
from jax.experimental import pallas as pl
from jax.experimental.pallas import tpu as pltpu
from jax.sharding import PartitionSpec as P

N, D, FF = 4096, 768, 2048
C, NC = 256, 8
WIDE, BOTH = 2 * C, 2 * FF
QUARTER, PIECE, HALF = C // 2, C // 4, C // 8
ROWS = D // NC
UNITS = 24
PER = UNITS // 2
DOWNS = (NC, PER + 1)
LAST = 17
OTHERS = (1, 2, 3)
SENT, CAME, LINE = 5, 6, 3
T0, T1, T2, T3, T4, T5 = FF, WIDE, FF, WIDE, FF, WIDE
S0, S1, S2, S3, S4 = 4, 2, 4, 2, 4
M3 = 4
f32, bf16 = jnp.float32, jnp.bfloat16
NN = (((1,), (0,)), ((), ()))
NT = (((1,), (1,)), ((), ()))
TN = (((0,), (0,)), ((), ()))
MESH = pl.DeviceIdType.MESH
VMEM, SEM = pltpu.VMEM, pltpu.SemaphoreType.DMA
PAIR = SEM((2,))
local = pltpu.make_async_copy


def dot(a, b, dims=NN):
    return lax.dot_general(a, b, dims, preferred_element_type=f32)


def scale_of(wide):
    return lax.rsqrt(jnp.mean(wide * wide, -1, keepdims=True) + 1e-6)


def normed(h):
    wide = h.astype(f32)
    return (wide * scale_of(wide)).astype(bf16)


def norm_back(h, by_a, by_out):
    wide = h.astype(f32)
    by_a = by_a.astype(bf16).astype(f32)
    scale = scale_of(wide)
    along = jnp.mean(by_a * wide, -1, keepdims=True) * (scale * scale * scale)
    return (by_out.astype(f32) + (by_a * scale - wide * along).astype(bf16).astype(f32)).astype(bf16)


def back(g, u, dp):
    dp = dp.astype(bf16).astype(f32)
    s = jax.nn.sigmoid(g)
    sg = g * s
    return jnp.concatenate([(dp * u * (s + sg * (1 - s))).astype(bf16), (dp * sg).astype(bf16)], 1), sg * u


def times(start, size):
    return pl.ds(pl.multiple_of(start * size, size), size)


def loop(count, body):
    def step(i, carry):
        body(i)
        return carry

    lax.fori_loop(0, count, step, 0)


def fetch(i, count, copies, started=False):
    @pl.when((i == 0) & (not started))
    def _():
        for c in copies(i):
            c.start()

    @pl.when(i + 1 < count)
    def _():
        for c in copies(i + 1):
            c.start()


def arrive(copies):
    for c in copies:
        c.wait()


def again(i, copy):
    pl.when(i >= 2)(copy.wait)


def gates(ref, layer, cols=slice(None)):
    w = ref[layer, :, :, :, cols]
    return w.reshape(D, w.shape[-1])


def choose(i, cases, low=0):
    if len(cases) == 1:
        return cases[0]()
    half = len(cases) // 2
    pl.when(i < low + half)(lambda: choose(i, cases[:half], low))
    pl.when(i >= low + half)(lambda: choose(i, cases[half:], low + half))


def added(t, ref, term):
    return jnp.where(t == 0, 0.0, ref) + term


def kernel(x, dy, wg, wu, wd, dx, og, ou, od, gus, ps, dgus, h1s, a0s, dws, A, DY, WGU, WD, lsem, go):
    x_in, dy_in = local(x, A, lsem.at[0]), local(dy, DY, lsem.at[1])
    a_out, a_in = local(A, a0s, lsem.at[0]), local(a0s, A, lsem.at[0])
    go.own(0)
    x_in.start()
    go.open()
    x_in.wait()

    @functools.partial(loop, N // C)
    def _(t):
        A[times(t, C), :] = normed(A[times(t, C), :])

    a_out.start()
    go.weights_first()
    dy_in.start()

    def forward(hid, stg, st, sp, ss, sx, sh):
        x_tile = states_in(st, sx)
        arrive_later = x_tile(0)
        for c in arrive_later:
            c.start()
        kept = hidden0(hid, stg, ss)
        a_out.wait()
        local(hid, ps, sp).start()
        states1(hid, st, x_tile, sh)
        arrive(kept)
        local(hid, ps, sp).wait()

    def states_in(st, sx):
        return lambda t: [local(x.at[times(t, T1)], st.at[t % 3], sx.at[t % 3])]

    def hidden0(hid, stg, ss):
        B, nt = T0 // S0, N // T0

        def leave(it):
            return local(stg.at[it % 2], gus.at[it // nt, times(it % nt, T0)], ss.at[it % 2])

        def tile(it):
            j, t, slot = it // nt, it % nt, it % 2
            again(it, leave(it))
            go.step0(it)
            w = gates(WGU, 0, times(j, WIDE))
            for k in range(S0):
                gu = dot(A[pl.ds(t * T0 + k * B, B), :], w)
                stg[slot, pl.ds(k * B, B)] = gu
                g, u = gu[:, :C], gu[:, C:]
                hid[pl.ds(t * T0 + k * B, B), times(j, C)] = (g * jax.nn.sigmoid(g) * u).astype(bf16)
            leave(it).start()

        loop(NC * nt, tile)
        return map(leave, range(2))

    def states1(hid, st, come, ss):
        B, nt = T1 // S1, N // T1

        def leave(t):
            return local(st.at[t % 3], h1s.at[times(t, T1)], ss.at[t % 3])

        def tile(t):
            slot = t % 3
            pl.when(t >= 2)(lambda: leave(t - 2).wait())
            fetch(t, nt, come, True)
            arrive(come(t))
            go.step1(t)
            for k in range(S1):
                m = dot(hid[pl.ds(t * T1 + k * B, B), :], WD[0].reshape(FF, D)).astype(bf16)
                h = (st[slot, pl.ds(k * B, B)].astype(f32) + m.astype(f32)).astype(bf16)
                st[slot, pl.ds(k * B, B)] = h
                A[pl.ds(t * T1 + k * B, B), :] = normed(h)
            leave(t).start()

        loop(nt, tile)
        arrive(map(leave, range(nt - 2, nt)))

    pl.run_scoped(forward, VMEM((N, FF), bf16), VMEM((2, T0, WIDE), f32), VMEM((3, T1, D), bf16), SEM, PAIR, SEM((3,)), SEM((3,)))

    def backward(ACC, *sums):
        go.sums(ACC, *sums)
        dy_in.wait()

        def last_layer(acc, stg, ss, sd):
            B, nt = T2 // S2, N // T2

            def leave(it):
                return local(stg.at[it % 2], dgus.at[times(it % nt, T2), times(it // nt, WIDE)], ss.at[it % 2])

            def leave_down(j):
                return local(acc.at[j % 2], dws.at[j], sd.at[j % 2])

            def tile(it):
                j, t, slot, here = it // nt, it % nt, it % 2, it // nt % 2
                r = times(t, T2)
                again(it, leave(it))
                pl.when((t == 0) & (j >= 2))(leave_down(j).wait)
                go.step2(j, t)
                w, wdn = gates(WGU, 1, times(j, WIDE)), WD[1, j // 2, j % 2]
                dgu, p = [], []
                for k in range(S2):
                    rr = pl.ds(t * T2 + k * B, B)
                    gu = dot(A[rr, :], w)
                    by_gu, hidden = back(gu[:, :C], gu[:, C:], dot(DY[rr, :], wdn, NT))
                    stg[slot, pl.ds(k * B, B)] = by_gu
                    dgu.append(by_gu)
                    p.append(hidden.astype(bf16))
                ACC[here] = added(t, ACC[here], dot(A[r, :], jnp.concatenate(dgu), TN).reshape(NC, ROWS, WIDE))
                acc[here] = added(t, acc[here], dot(jnp.concatenate(p), DY[r, :], TN))
                leave(it).start()

                @pl.when(t == nt - 1)
                def _():
                    leave_down(j).start()
                    go.end2(j)

            loop(NC * nt, tile)
            arrive(map(leave, range(2)))
            arrive(map(leave_down, range(2)))

        pl.run_scoped(last_layer, VMEM((2, C, D), f32), VMEM((2, T2, WIDE), bf16), PAIR, PAIR)

        def first_layer(acc, sl):
            go.downs(acc, sl)

            def between(sg, sp, sh, *sems):
                B, M, nt = T3 // S3, FF // M3, N // T3

                def come(t):
                    pairs = (dgus, sg), (ps, sp), (h1s, sh)
                    return [local(src.at[times(t, T3)], dst.at[t % 2], sem.at[t % 2]) for (src, dst), sem in zip(pairs, sems)]

                def tile(t):
                    slot = t % 2
                    fetch(t, nt, come)
                    pl.when(t == 0)(a_in.start)
                    arrive(come(t))
                    dh = []
                    for k in range(S3):
                        rr = pl.ds(t * T3 + k * B, B)
                        da = dot(sg[slot, pl.ds(k * B, B), :], gates(WGU, 1), NT)
                        dh.append(norm_back(sh[slot, pl.ds(k * B, B)], da, DY[rr, :]))
                        DY[rr, :] = dh[-1]
                    dh = jnp.concatenate(dh)
                    for m in range(M3):
                        c = pl.ds(m * M, M)
                        acc[c, :] = added(t, acc[c, :], dot(sp[slot, :, c], dh, TN))
                    go.step3(t)

                loop(nt, tile)

            pl.run_scoped(between, VMEM((2, T3, BOTH), bf16), VMEM((2, T3, FF), bf16), VMEM((2, T3, D), bf16), PAIR, PAIR, PAIR)

            def chunks(stg, sin, ss, si):
                B, nt = T4 // S4, N // T4

                def come(it):
                    return [local(gus.at[it // nt, times(it % nt, T4)], sin.at[it % 2], si.at[it % 2])]

                def leave(it):
                    return local(stg.at[it % 2], dgus.at[times(it % nt, T4), times(it // nt, WIDE)], ss.at[it % 2])

                def tile(it):
                    j, t, slot = it // nt, it % nt, it % 2
                    fetch(it, NC * nt, come)
                    again(it, leave(it))
                    go.step4(it)
                    arrive(come(it))
                    wdn = WD[0, j // 2, j % 2]
                    dgu = []
                    for k in range(S4):
                        dp = dot(DY[pl.ds(t * T4 + k * B, B), :], wdn, NT)
                        gu = sin[slot, pl.ds(k * B, B), :]
                        by_gu, _ = back(gu[:, :C], gu[:, C:], dp)
                        stg[slot, pl.ds(k * B, B)] = by_gu
                        dgu.append(by_gu)
                    ACC[j % 2] = added(t, ACC[j % 2], dot(A[times(t, T4), :], jnp.concatenate(dgu), TN).reshape(NC, ROWS, WIDE))
                    leave(it).start()

                loop(NC * nt, tile)
                arrive(map(leave, range(2)))

            a_in.wait()
            pl.run_scoped(chunks, VMEM((2, T4, WIDE), bf16), VMEM((2, T4, WIDE), f32), PAIR, PAIR)

        pl.run_scoped(first_layer, VMEM((FF, D), f32), SEM)

        def last(sg, sh, so, pending, ss, *sems):
            B, nt = T5 // 2, N // T5

            def come(t):
                pairs = (dgus, sg, 2), (x, sh, 3)
                return [local(src.at[times(t, T5)], dst.at[t % k], sem.at[t % k]) for (src, dst, k), sem in zip(pairs, sems)]

            def leave(t):
                return local(so.at[t % 3], dx.at[times(t, T5)], ss.at[t % 3])

            def finish(slot, t, part, da):
                so[slot, times(part, B)] = norm_back(sh[slot, times(part, B)], da, DY[pl.ds(t * T5 + part * B, B), :])

            def tile(t):
                fetch(t, nt, come)
                pl.when(t >= 3)(leave(t).wait)
                go.step5(t)
                arrive(come(t))
                finish((t + 2) % 3, (t + nt - 1) % nt, 1, pending[...])
                by_a = [dot(sg[t % 2, times(k, B), :], gates(WGU, 0), NT) for k in range(2)]
                finish(t % 3, t, 0, by_a[0])
                pending[...] = by_a[1]
                pl.when(t >= 1)(lambda: leave(t - 1).start())

            loop(nt, tile)
            finish((nt - 1) % 3, nt - 1, 1, pending[...])
            leave(nt - 1).start()
            arrive(map(leave, range(nt - 3, nt)))

        pl.run_scoped(
            last,
            VMEM((2, T5, BOTH), bf16),
            VMEM((3, T5, D), bf16),
            VMEM((3, T5, D), bf16),
            VMEM((T5 // 2, D), f32),
            SEM((3,)),
            PAIR,
            SEM((3,)),
        )
        go.close()

    pl.run_scoped(backward, VMEM((2, NC, ROWS, WIDE), f32), *go.scratch())


class Links:
    def __init__(self, wg, wu, wd, og, ou, od, dws, WGU, WD, CR, XR, ZR, wsem, csem, xsem, zsem, osem, cred):
        self.wg, self.wu, self.wd, self.outs, self.od, self.dws, self.WGU, self.WD = wg, wu, wd, (og, ou), od, dws, WGU, WD
        self.CR, self.XR, self.ZR = CR, XR, ZR
        self.wsem, self.csem, self.xsem, self.zsem, self.osem, self.cred = wsem, csem, xsem, zsem, osem, cred
        s, z = lax.axis_index("s"), lax.axis_index("r")
        self.z, self.s = z, s
        x, y, c = s // 4, s // 2 % 2, s % 2
        self.core, self.chip = c, s // 2
        self.chips = 2 * (1 - x) + y, 2 * x + 1 - y, 2 * (1 - x) + 1 - y
        self.planes = [2 * q + c for q in self.chips]
        self.partner = s + 1 - 2 * c
        self.lines = z + 1 - 2 * (z % 2), (z + 2) % 4

    def to(self, s=None, z=None):
        return (0, self.z if z is None else z, self.s if s is None else s)

    def remote(self, src, dst, send, recv, to):
        pltpu.make_async_remote_copy(src, dst, send, recv, device_id=to, device_id_type=MESH).start()

    def done(self, ref, sem):
        local(ref, ref, sem).wait()


    def kind(self, u):
        if not isinstance(u, int):
            return 1, True, u - LAST + 1
        layer, v = u // PER, u % PER
        if layer == 0:
            return layer, v < NC, v % NC
        return layer, v == 0 or v > 4, v - 4 if v > 4 else max(v - 1, 0)

    def unit(self, u, chip, core, rows=None):
        layer, gate, k = self.kind(u)
        if gate:
            return self.WGU.at[layer, chip, core, rows or slice(None), times(k, WIDE)]
        start, size = (rows.start, rows.size) if rows else (0, PIECE)
        return self.WD.at[layer, chip, core, pl.ds(k * PIECE + start, size), :]

    def own(self, u):
        layer, gate, k = self.kind(u)
        sem = self.wsem.at[0, u]
        if gate:
            for w, side in ((self.wg, 0), (self.wu, C)):
                local(w.at[layer, :, pl.ds(k * C, C)], self.WGU.at[layer, self.chip, self.core, :, pl.ds(k * WIDE + side, C)], sem).start()
        elif k == 0:
            local(self.wd.at[layer], self.WD.at[layer, self.chip, self.core], sem).start()

    def first(self, u):
        layer, gate, k = self.kind(u)
        mine = self.unit(u, self.chip, self.core)
        if gate:
            self.done(mine, self.wsem.at[0, u])
        elif k == 0:
            self.done(self.WD.at[layer, self.chip, self.core], self.wsem.at[0, u])
        for to in self.planes[:2]:
            self.remote(mine, mine, self.wsem.at[1, u], self.wsem.at[2, u], self.to(to))

    def second(self, u):
        self.done(self.unit(u, 0, pl.ds(0, 2)), self.wsem.at[2, u])
        size = (ROWS if self.kind(u)[1] else PIECE) // 2
        for half in range(2):
            ref = self.unit(u, self.chips[half], self.core, pl.ds(half * size, size))
            self.remote(ref, ref, self.wsem.at[1, u], self.wsem.at[3, u], self.to(self.planes[1 - half]))

    def third(self, u):
        self.done(self.unit(u, 0, 0), self.wsem.at[3, u])
        ref = self.unit(u, slice(None), self.core)
        self.remote(ref, ref, self.wsem.at[5, u], self.wsem.at[4, u], self.to(self.partner))

    def whole(self, u):
        self.done(self.unit(u, slice(None), 0), self.wsem.at[4, u])

    def pass_on(self, it):
        for u in range(2, LAST):
            if (5 * u - 6) // 3 == it:
                self.second(u)
                self.first(u + 2)
        for u in range(1, LAST):
            if 5 * u // 3 == it:
                self.third(u)

    def open(self):
        self.own(1)
        barrier = pltpu.get_barrier_semaphore()
        peers = [self.to(self.partner)] + [self.to(s) for s in self.planes] + [self.to(z=z) for z in self.lines]
        for peer in peers:
            pl.semaphore_signal(barrier, inc=1, device_id=peer, device_id_type=MESH)
        pl.semaphore_wait(barrier, len(peers))
        self.first(0)
        self.first(1)
        for u in range(2, NC + 1):
            self.own(u)

    def weights_first(self):
        self.second(0)
        self.first(2)
        self.second(1)
        self.first(3)
        self.third(0)

    def step0(self, it):
        def case(k):
            self.pass_on(k)
            if k % 2 == 0:
                self.whole(k // 2)
            if PER + k < UNITS:
                self.own(PER + k)

        choose(it, [functools.partial(case, k) for k in range(2 * NC)])

    def step1(self, t):
        def case(k):
            if k == 0:
                self.pass_on(2 * NC)
                self.pass_on(2 * NC + 1)
                for u in range(NC, PER):
                    if 5 * u // 3 >= 2 * NC + 2:
                        self.third(u)
                for u in range(NC, PER):
                    self.whole(u)
            for u in range(PER, LAST):
                if (5 * u - 6) // 3 == k + 2 * NC + 2:
                    self.second(u)
                    self.first(u + 2)
                if 5 * u // 3 == k + 2 * NC + 2:
                    self.third(u)

        choose(t, [functools.partial(case, k) for k in range(NC)])


    @staticmethod
    def scratch():
        blocks, wide = (4, ROWS, WIDE), (ROWS, WIDE)
        return (
            VMEM((2, *blocks), bf16),
            VMEM((SENT, 3, *wide), bf16),
            VMEM((CAME, *wide), f32),
            VMEM((2, LINE, *wide), bf16),
            VMEM((2, *wide), bf16),
            VMEM((2, PIECE, D), bf16),
        )

    def sums(self, ACC, CS, XS, O2, ZS, F, FD):
        self.ACC, self.CS, self.XS, self.O2, self.ZS, self.F, self.FD = ACC, CS, XS, O2, ZS, F, FD

    def free(self, k, to):
        pl.semaphore_signal(self.cred.at[k], inc=1, device_id=to, device_id_type=MESH)

    def pack(self, n, block):
        b = n % 2
        for chip in range(4):
            self.CS[b, chip] = block(2 * chip + 1 - self.core).astype(bf16)

        @pl.when(n >= 2)
        def _():
            pl.semaphore_wait(self.cred.at[0], 1)

        self.remote(self.CS.at[b], self.CR.at[b], self.csem.at[0, b], self.csem.at[1, b], self.to(self.partner))

    def pack_gate(self, n, slot):
        self.pack(n, lambda s: self.ACC[slot, s])

    def plane_gate(self, n, slot):
        self.plane(n, lambda s: self.ACC[slot, s])

    def downs(self, acc, sem):
        self.acc, self.acc_sem = acc, sem
        self.load_down(0)

    def load_down(self, k):
        for b in range(3):
            for h in range(2):
                src = self.dws.at[:, pl.ds(pl.multiple_of(k * PIECE + h * HALF, HALF), HALF), pl.ds(b * C, C)]
                local(src, self.ACC.at[k % 2, :, pl.ds(b * HALF, HALF), pl.ds(h * C, C)], self.acc_sem).start()

    def pack_down1(self, n):
        self.done(self.ACC.at[n % 2], self.acc_sem)
        self.pack_gate(n, n % 2)
        pl.when(n < PER - 1)(lambda: self.load_down(n - NC + 1))

    def down0(self, k):
        def block(s):
            rows = []
            for b in range(3):
                sides = [self.acc[pl.ds(pl.multiple_of(s * C + k * PIECE + h * HALF, HALF), HALF), pl.ds(b * C, C)] for h in range(2)]
                rows.append(jnp.concatenate(sides, 1))
            return jnp.concatenate(rows)

        return block

    def plane(self, n, block):
        b, xs, xb = n % 2, n % SENT, n % CAME
        for side, ref in enumerate((self.CS, self.CR)):
            self.done(ref.at[b], self.csem.at[side, b])

        def total(chip):
            return block(2 * chip + self.core) + self.CR[b, chip].astype(f32)

        for m, chip in enumerate(self.chips):
            self.XS[xs, m] = total(chip).astype(bf16)
        self.O2[xb] = total(self.chip)
        pl.when(n + 2 < UNITS)(lambda: self.free(0, self.to(self.partner)))

        @pl.when(n >= CAME)
        def _():
            for m in OTHERS:
                pl.semaphore_wait(self.cred.at[m], 1)

        for m, s in enumerate(self.planes):
            self.remote(self.XS.at[xs, m], self.XR.at[xb, m], self.xsem.at[0, xs], self.xsem.at[1, xb], self.to(s))

    def line(self, n, k, total):
        zb = n % LINE
        self.ZS[k, zb] = total.astype(bf16)

        @pl.when(n >= LINE)
        def _():
            pl.semaphore_wait(self.cred.at[4 + k], 1)

        self.remote(self.ZS.at[k, zb], self.ZR.at[k, zb], self.zsem.at[k, 0, zb], self.zsem.at[k, 1, zb], self.to(z=self.lines[k]))

    def line_sum(self, n, k):
        zb = n % LINE
        for side, ref in enumerate((self.ZS, self.ZR)):
            self.done(ref.at[k, zb], self.zsem.at[k, side, zb])
        total = self.ZS[k, zb].astype(f32) + self.ZR[k, zb].astype(f32)
        pl.when(n + LINE < UNITS)(lambda: self.free(4 + k, self.to(z=self.lines[k])))
        return total

    def line1(self, n):
        xs, xb = n % SENT, n % CAME
        self.done(self.XS.at[xs], self.xsem.at[0, xs])
        self.done(self.XR.at[xb], self.xsem.at[1, xb])
        total = self.O2[xb] + (self.XR[xb, 0].astype(f32) + self.XR[xb, 1].astype(f32) + self.XR[xb, 2].astype(f32))

        @pl.when(n + CAME < UNITS)
        def _():
            for m, s in zip(OTHERS, self.planes):
                self.free(m, self.to(s))

        self.line(n, 0, total)

    def line2(self, n):
        self.line(n, 1, self.line_sum(n, 0))

    def finish(self, n):
        total = self.line_sum(n, 1).astype(bf16)
        pl.when(n >= 2)(lambda: self.done(self.F.at[n % 2], self.osem.at[n % 2]))
        return total

    def final_gate(self, n, layer, j):
        b = n % 2
        self.F[b] = self.finish(n)
        for side, out in enumerate(self.outs):
            local(self.F.at[b, :, pl.ds(side * C, C)], out.at[layer, :, times(j, C)], self.osem.at[b]).start()

    def final_down(self, n, layer, k):
        b = n % 2
        total = self.finish(n)
        for i in range(3):
            for h in range(2):
                self.FD[b, pl.ds(h * HALF, HALF), pl.ds(i * C, C)] = total[i * HALF : (i + 1) * HALF, h * C : (h + 1) * C]
        local(self.FD.at[b], self.od.at[layer, times(k, PIECE)], self.osem.at[b]).start()

    def final1(self, n):
        self.final_gate(n, 1, n)

    def step2(self, j, t):
        @pl.when(t == 0)
        def _():
            @pl.when(j == 0)
            def _():
                self.third(LAST - 1)
                for u in range(PER, LAST):
                    self.whole(u)

            pl.when(j >= 1)(lambda: self.whole(LAST - 1 + j))
            pl.when(j < UNITS - LAST)(lambda: self.second(LAST + j))
            pl.when(j < UNITS - LAST - 2)(lambda: self.first(LAST + 2 + j))

        @pl.when(t == 1)
        def _():
            pl.when(j < UNITS - LAST)(lambda: self.third(LAST + j))
            pl.when(j >= 1)(lambda: self.plane_gate(j - 1, (j - 1) % 2))
            for back, stage in enumerate((self.line1, self.line2, self.final1), 2):
                pl.when(j >= back)(functools.partial(stage, j - back))

    def end2(self, j):
        self.pack_gate(j, j % 2)

    def step3(self, t):
        pl.when(t <= 3)(lambda: self.final1(4 + t))
        pl.when(t >= 6)(lambda: self.final_down(2 + t, 1, t - 6))
        pl.when(t <= 2)(lambda: self.line2(5 + t))
        pl.when(t >= 4)(lambda: self.line2(4 + t))
        pl.when(t <= 1)(lambda: self.line1(6 + t))
        pl.when((t >= 3) & (t <= 6))(lambda: self.line1(5 + t))
        pl.when(t <= 4)(lambda: self.plane_gate(7 + t, (7 + t) % 2))
        pl.when(t <= 3)(lambda: self.pack_down1(8 + t))

    def step4(self, it):
        pl.when(it <= 1)(lambda: self.final_down(PER - 2 + it, 1, 2 + it))
        pl.when((it == 11) | (it == 14))(lambda: self.final_down(PER + (it - 11) // 3 * 2, 0, (it - 11) // 3))
        pl.when(it == 13)(lambda: self.final_gate(PER + 1, 0, 0))
        for start, stage in ((8, self.line2), (6, self.line1)):
            @pl.when((it >= start) & ((it - start) % 3 != 1))
            def _():
                stage(PER + (2 * (it - start) + 1) // 3)

        @pl.when(it % 2 == 0)
        def _():
            j = it // 2 - 1

            @pl.when((j >= 0) & (j <= 3))
            def _():
                self.plane(PER + it - 2, self.down0(j))
                self.pack_gate(PER + it - 1, j % 2)

            pl.when(j >= 4)(lambda: self.pack_gate(2 * NC + j, j % 2))

        @pl.when(it % 2 == 1)
        def _():
            k = it // 2
            pl.when((k >= 1) & (k <= 4))(lambda: self.plane_gate(PER + it - 2, (k - 1) % 2))
            pl.when(k >= 5)(lambda: self.plane_gate(2 * NC + k - 1, (k - 1) % 2))
            pl.when(k <= 3)(lambda: self.pack(PER + it - 1, self.down0(k)))

    def step5(self, t):
        pl.when((t == 1) | (t == 3))(lambda: self.final_down(PER + 3 + t, 0, (t + 3) // 2))
        pl.when((t == 0) | (t == 2))(lambda: self.final_gate(PER + 3 + t, 0, t // 2 + 1))
        pl.when(t >= 4)(lambda: self.final_gate(PER + 3 + t, 0, t - 1))
        pl.when(t <= 6)(lambda: self.line2(PER + 5 + t))
        pl.when(t <= 4)(lambda: self.line1(PER + 7 + t))
        pl.when(t == 1)(lambda: self.plane_gate(UNITS - 1, 1))
        pl.when(t == 0)(lambda: self.pack_gate(UNITS - 1, 1))

    def close(self):
        self.final_gate(UNITS - 1, 0, NC - 1)
        for b in range(2):
            self.done(self.F.at[b], self.osem.at[b])
        for u in range(UNITS):
            self.done(self.unit(u, pl.ds(0, 3), 0), self.wsem.at[1, u])
            self.done(self.unit(u, slice(None), 0), self.wsem.at[5, u])


def whole(x, dy, wg, wu, wd, dx, og, ou, od, gus, ps, dgus, h1s, a0s, dws, A, DY, WGU, WD, CR, XR, ZR, lsem, wsem, csem, xsem, zsem, osem, cred):
    links = Links(wg, wu, wd, og, ou, od, dws, WGU, WD, CR, XR, ZR, wsem, csem, xsem, zsem, osem, cred)
    kernel(x, dy, wg, wu, wd, dx, og, ou, od, gus, ps, dgus, h1s, a0s, dws, A, DY, WGU, WD, lsem, links)


def solution(mesh):
    def call(x, dy, wg, wu, wd):
        anywhere = pl.BlockSpec(memory_space=pl.ANY)
        S, V, M = jax.ShapeDtypeStruct, VMEM, SEM
        flops = 17 * 2 * N * D * FF
        out = pl.pallas_call(
            whole,
            in_specs=[anywhere] * 5,
            out_specs=[anywhere] * 10,
            out_shape=[
                S((N, D), bf16),
                S((2, ROWS, FF), bf16),
                S((2, ROWS, FF), bf16),
                S((2, C, D), bf16),
                S((NC, N, WIDE), f32),
                S((N, FF), bf16),
                S((N, BOTH), bf16),
                S((N, D), bf16),
                S((N, D), bf16),
                S((NC, C, D), f32),
            ],
            scratch_shapes=[
                V((N, D), bf16),
                V((N, D), bf16),
                V((2, 4, 2, ROWS, BOTH), bf16),
                V((2, 4, 2, C, D), bf16),
                V((2, 4, ROWS, WIDE), bf16),
                V((CAME, 3, ROWS, WIDE), bf16),
                V((2, LINE, ROWS, WIDE), bf16),
                PAIR,
                M((6, UNITS)),
                M((2, 2)),
                M((2, CAME)),
                M((2, 2, LINE)),
                PAIR,
                pltpu.SemaphoreType.REGULAR((6,)),
            ],
            compiler_params=pltpu.CompilerParams(vmem_limit_bytes=67_000_000, collective_id=0, has_side_effects=True),
            cost_estimate=pl.CostEstimate(flops=flops, bytes_accessed=400_000_000, transcendentals=0),
            name="stack",
        )(x, dy, wg, wu, wd)
        return out[:4]

    def step(x, dy, wg, wu, wd):
        dx, *by_weights = call(x[0], dy[0], wg, wu, wd)
        return dx[None], *by_weights

    states, cut = P(("rep", "r", "s"), None, None), P(None, "s", None)
    return jax.shard_map(
        step,
        mesh=mesh,
        in_specs=(states, states) + (cut,) * 3,
        out_specs=(states,) + (P("rep", "s", None),) * 3,
        check_vma=False,
    )
```

```python
import functools

import jax
import jax.numpy as jnp
from jax import lax
from jax.experimental import pallas as pl
from jax.experimental.pallas import tpu as pltpu
from jax.sharding import PartitionSpec as P

N, D, FF = 4096, 768, 2048
C, NC = 256, 8
WIDE, BOTH = 2 * C, 2 * FF
QUARTER, PIECE, HALF = C // 2, C // 4, C // 8
ROWS = D // NC
UNITS = 24
PER = UNITS // 2
DOWNS = (NC, PER + 1)
LAST = 17
OTHERS = (1, 2, 3)
SENT, CAME, LINE = 5, 6, 3
T0, T1, T2, T3, T4, T5 = FF, WIDE, FF, WIDE, FF, WIDE
S0, S1, S2, S3, S4 = 4, 2, 4, 2, 4
M3 = 4
f32, bf16 = jnp.float32, jnp.bfloat16
NN = (((1,), (0,)), ((), ()))
NT = (((1,), (1,)), ((), ()))
TN = (((0,), (0,)), ((), ()))
MESH = pl.DeviceIdType.MESH
VMEM, SEM = pltpu.VMEM, pltpu.SemaphoreType.DMA
PAIR = SEM((2,))
local = pltpu.make_async_copy


def dot(a, b, dims=NN):
    return lax.dot_general(a, b, dims, preferred_element_type=f32)


def scale_of(wide):
    return lax.rsqrt(jnp.mean(wide * wide, -1, keepdims=True) + 1e-6)


def normed(h):
    wide = h.astype(f32)
    return (wide * scale_of(wide)).astype(bf16)


def norm_back(h, by_a, by_out):
    wide = h.astype(f32)
    by_a = by_a.astype(bf16).astype(f32)
    scale = scale_of(wide)
    along = jnp.mean(by_a * wide, -1, keepdims=True) * (scale * scale * scale)
    return (by_out.astype(f32) + (by_a * scale - wide * along).astype(bf16).astype(f32)).astype(bf16)


def back(g, u, dp):
    dp = dp.astype(bf16).astype(f32)
    s = jax.nn.sigmoid(g)
    sg = g * s
    return jnp.concatenate([(dp * u * (s + sg * (1 - s))).astype(bf16), (dp * sg).astype(bf16)], 1), sg * u


def times(start, size):
    return pl.ds(pl.multiple_of(start * size, size), size)


def loop(count, body):
    def step(i, carry):
        body(i)
        return carry

    lax.fori_loop(0, count, step, 0)


def fetch(i, count, copies, started=False):
    @pl.when((i == 0) & (not started))
    def _():
        for c in copies(i):
            c.start()

    @pl.when(i + 1 < count)
    def _():
        for c in copies(i + 1):
            c.start()


def arrive(copies):
    for c in copies:
        c.wait()


def again(i, copy):
    pl.when(i >= 2)(copy.wait)


def gates(ref, layer, cols=slice(None)):
    w = ref[layer, :, :, :, cols]
    return w.reshape(D, w.shape[-1])


def choose(i, cases, low=0):
    if len(cases) == 1:
        return cases[0]()
    half = len(cases) // 2
    pl.when(i < low + half)(lambda: choose(i, cases[:half], low))
    pl.when(i >= low + half)(lambda: choose(i, cases[half:], low + half))


def added(t, ref, term):
    return jnp.where(t == 0, 0.0, ref) + term


def kernel(x, dy, wg, wu, wd, dx, og, ou, od, gus, ps, dgus, h1s, a0s, dws, A, DY, WGU, WD, lsem, go):
    x_in, dy_in = local(x, A, lsem.at[0]), local(dy, DY, lsem.at[1])
    a_out, a_in = local(A, a0s, lsem.at[0]), local(a0s, A, lsem.at[0])
    go.own(0)
    x_in.start()
    go.open()
    x_in.wait()

    @functools.partial(loop, N // C)
    def _(t):
        A[times(t, C), :] = normed(A[times(t, C), :])

    a_out.start()
    go.weights_first()
    dy_in.start()

    def forward(hid, stg, st, sp, ss, sx, sh):
        x_tile = states_in(st, sx)
        arrive_later = x_tile(0)
        for c in arrive_later:
            c.start()
        kept = hidden0(hid, stg, ss)
        a_out.wait()
        local(hid, ps, sp).start()
        states1(hid, st, x_tile, sh)
        arrive(kept)
        local(hid, ps, sp).wait()

    def states_in(st, sx):
        return lambda t: [local(x.at[times(t, T1)], st.at[t % 3], sx.at[t % 3])]

    def hidden0(hid, stg, ss):
        B, nt = T0 // S0, N // T0

        def leave(it):
            return local(stg.at[it % 2], gus.at[it // nt, times(it % nt, T0)], ss.at[it % 2])

        def tile(it):
            j, t, slot = it // nt, it % nt, it % 2
            again(it, leave(it))
            go.step0(it)
            w = gates(WGU, 0, times(j, WIDE))
            for k in range(S0):
                gu = dot(A[pl.ds(t * T0 + k * B, B), :], w)
                stg[slot, pl.ds(k * B, B)] = gu
                g, u = gu[:, :C], gu[:, C:]
                hid[pl.ds(t * T0 + k * B, B), times(j, C)] = (g * jax.nn.sigmoid(g) * u).astype(bf16)
            leave(it).start()

        loop(NC * nt, tile)
        return map(leave, range(2))

    def states1(hid, st, come, ss):
        B, nt = T1 // S1, N // T1

        def leave(t):
            return local(st.at[t % 3], h1s.at[times(t, T1)], ss.at[t % 3])

        def tile(t):
            slot = t % 3
            pl.when(t >= 2)(lambda: leave(t - 2).wait())
            fetch(t, nt, come, True)
            arrive(come(t))
            go.step1(t)
            for k in range(S1):
                m = dot(hid[pl.ds(t * T1 + k * B, B), :], WD[0].reshape(FF, D)).astype(bf16)
                h = (st[slot, pl.ds(k * B, B)].astype(f32) + m.astype(f32)).astype(bf16)
                st[slot, pl.ds(k * B, B)] = h
                A[pl.ds(t * T1 + k * B, B), :] = normed(h)
            leave(t).start()

        loop(nt, tile)
        arrive(map(leave, range(nt - 2, nt)))

    pl.run_scoped(forward, VMEM((N, FF), bf16), VMEM((2, T0, WIDE), f32), VMEM((3, T1, D), bf16), SEM, PAIR, SEM((3,)), SEM((3,)))

    def backward(ACC, *sums):
        go.sums(ACC, *sums)
        dy_in.wait()

        def last_layer(acc, stg, ss, sd):
            B, nt = T2 // S2, N // T2

            def leave(it):
                return local(stg.at[it % 2], dgus.at[times(it % nt, T2), times(it // nt, WIDE)], ss.at[it % 2])

            def leave_down(j):
                return local(acc.at[j % 2], dws.at[j], sd.at[j % 2])

            def tile(it):
                j, t, slot, here = it // nt, it % nt, it % 2, it // nt % 2
                r = times(t, T2)
                again(it, leave(it))
                pl.when((t == 0) & (j >= 2))(leave_down(j).wait)
                go.step2(j, t)
                w, wdn = gates(WGU, 1, times(j, WIDE)), WD[1, j // 2, j % 2]
                dgu, p = [], []
                for k in range(S2):
                    rr = pl.ds(t * T2 + k * B, B)
                    gu = dot(A[rr, :], w)
                    by_gu, hidden = back(gu[:, :C], gu[:, C:], dot(DY[rr, :], wdn, NT))
                    stg[slot, pl.ds(k * B, B)] = by_gu
                    dgu.append(by_gu)
                    p.append(hidden.astype(bf16))
                ACC[here] = added(t, ACC[here], dot(A[r, :], jnp.concatenate(dgu), TN).reshape(NC, ROWS, WIDE))
                acc[here] = added(t, acc[here], dot(jnp.concatenate(p), DY[r, :], TN))
                leave(it).start()

                @pl.when(t == nt - 1)
                def _():
                    leave_down(j).start()
                    go.end2(j)

            loop(NC * nt, tile)
            arrive(map(leave, range(2)))
            arrive(map(leave_down, range(2)))

        pl.run_scoped(last_layer, VMEM((2, C, D), f32), VMEM((2, T2, WIDE), bf16), PAIR, PAIR)

        def first_layer(acc, sl):
            go.downs(acc, sl)

            def between(sg, sp, sh, *sems):
                B, M, nt = T3 // S3, FF // M3, N // T3

                def come(t):
                    pairs = (dgus, sg), (ps, sp), (h1s, sh)
                    return [local(src.at[times(t, T3)], dst.at[t % 2], sem.at[t % 2]) for (src, dst), sem in zip(pairs, sems)]

                def tile(t):
                    slot = t % 2
                    fetch(t, nt, come)
                    pl.when(t == 0)(a_in.start)
                    arrive(come(t))
                    dh = []
                    for k in range(S3):
                        rr = pl.ds(t * T3 + k * B, B)
                        da = dot(sg[slot, pl.ds(k * B, B), :], gates(WGU, 1), NT)
                        dh.append(norm_back(sh[slot, pl.ds(k * B, B)], da, DY[rr, :]))
                        DY[rr, :] = dh[-1]
                    dh = jnp.concatenate(dh)
                    for m in range(M3):
                        c = pl.ds(m * M, M)
                        acc[c, :] = added(t, acc[c, :], dot(sp[slot, :, c], dh, TN))
                    go.step3(t)

                loop(nt, tile)

            pl.run_scoped(between, VMEM((2, T3, BOTH), bf16), VMEM((2, T3, FF), bf16), VMEM((2, T3, D), bf16), PAIR, PAIR, PAIR)

            def chunks(stg, sin, ss, si):
                B, nt = T4 // S4, N // T4

                def come(it):
                    return [local(gus.at[it // nt, times(it % nt, T4)], sin.at[it % 2], si.at[it % 2])]

                def leave(it):
                    return local(stg.at[it % 2], dgus.at[times(it % nt, T4), times(it // nt, WIDE)], ss.at[it % 2])

                def tile(it):
                    j, t, slot = it // nt, it % nt, it % 2
                    fetch(it, NC * nt, come)
                    again(it, leave(it))
                    go.step4(it)
                    arrive(come(it))
                    wdn = WD[0, j // 2, j % 2]
                    dgu = []
                    for k in range(S4):
                        dp = dot(DY[pl.ds(t * T4 + k * B, B), :], wdn, NT)
                        gu = sin[slot, pl.ds(k * B, B), :]
                        by_gu, _ = back(gu[:, :C], gu[:, C:], dp)
                        stg[slot, pl.ds(k * B, B)] = by_gu
                        dgu.append(by_gu)
                    ACC[j % 2] = added(t, ACC[j % 2], dot(A[times(t, T4), :], jnp.concatenate(dgu), TN).reshape(NC, ROWS, WIDE))
                    leave(it).start()

                loop(NC * nt, tile)
                arrive(map(leave, range(2)))

            a_in.wait()
            pl.run_scoped(chunks, VMEM((2, T4, WIDE), bf16), VMEM((2, T4, WIDE), f32), PAIR, PAIR)

        pl.run_scoped(first_layer, VMEM((FF, D), f32), SEM)

        def last(sg, sh, so, pending, ss, *sems):
            B, nt = T5 // 2, N // T5

            def come(t):
                pairs = (dgus, sg, 2), (x, sh, 3)
                return [local(src.at[times(t, T5)], dst.at[t % k], sem.at[t % k]) for (src, dst, k), sem in zip(pairs, sems)]

            def leave(t):
                return local(so.at[t % 3], dx.at[times(t, T5)], ss.at[t % 3])

            def finish(slot, t, part, da):
                so[slot, times(part, B)] = norm_back(sh[slot, times(part, B)], da, DY[pl.ds(t * T5 + part * B, B), :])

            def tile(t):
                fetch(t, nt, come)
                pl.when(t >= 3)(leave(t).wait)
                go.step5(t)
                arrive(come(t))
                finish((t + 2) % 3, (t + nt - 1) % nt, 1, pending[...])
                by_a = [dot(sg[t % 2, times(k, B), :], gates(WGU, 0), NT) for k in range(2)]
                finish(t % 3, t, 0, by_a[0])
                pending[...] = by_a[1]
                pl.when(t >= 1)(lambda: leave(t - 1).start())

            loop(nt, tile)
            finish((nt - 1) % 3, nt - 1, 1, pending[...])
            leave(nt - 1).start()
            arrive(map(leave, range(nt - 3, nt)))

        pl.run_scoped(
            last,
            VMEM((2, T5, BOTH), bf16),
            VMEM((3, T5, D), bf16),
            VMEM((3, T5, D), bf16),
            VMEM((T5 // 2, D), f32),
            SEM((3,)),
            PAIR,
            SEM((3,)),
        )
        go.close()

    pl.run_scoped(backward, VMEM((2, NC, ROWS, WIDE), f32), *go.scratch())


class Links:
    def __init__(self, wg, wu, wd, og, ou, od, dws, WGU, WD, CR, XR, ZR, wsem, csem, xsem, zsem, osem, cred):
        self.wg, self.wu, self.wd, self.outs, self.od, self.dws, self.WGU, self.WD = wg, wu, wd, (og, ou), od, dws, WGU, WD
        self.CR, self.XR, self.ZR = CR, XR, ZR
        self.wsem, self.csem, self.xsem, self.zsem, self.osem, self.cred = wsem, csem, xsem, zsem, osem, cred
        s, z = lax.axis_index("s"), lax.axis_index("r")
        self.z, self.s = z, s
        x, y, c = s // 4, s // 2 % 2, s % 2
        self.core, self.chip = c, s // 2
        self.chips = 2 * (1 - x) + y, 2 * x + 1 - y, 2 * (1 - x) + 1 - y
        self.planes = [2 * q + c for q in self.chips]
        self.partner = s + 1 - 2 * c
        self.lines = z + 1 - 2 * (z % 2), (z + 2) % 4

    def to(self, s=None, z=None):
        return (0, self.z if z is None else z, self.s if s is None else s)

    def remote(self, src, dst, send, recv, to):
        pltpu.make_async_remote_copy(src, dst, send, recv, device_id=to, device_id_type=MESH).start()

    def done(self, ref, sem):
        local(ref, ref, sem).wait()


    def kind(self, u):
        if not isinstance(u, int):
            return 1, True, u - LAST + 1
        layer, v = u // PER, u % PER
        if layer == 0:
            return layer, v < NC, v % NC
        return layer, v == 0 or v > 4, v - 4 if v > 4 else max(v - 1, 0)

    def unit(self, u, chip, core, rows=None):
        layer, gate, k = self.kind(u)
        if gate:
            return self.WGU.at[layer, chip, core, rows or slice(None), times(k, WIDE)]
        start, size = (rows.start, rows.size) if rows else (0, PIECE)
        return self.WD.at[layer, chip, core, pl.ds(k * PIECE + start, size), :]

    def own(self, u):
        layer, gate, k = self.kind(u)
        sem = self.wsem.at[0, u]
        if gate:
            for w, side in ((self.wg, 0), (self.wu, C)):
                local(w.at[layer, :, pl.ds(k * C, C)], self.WGU.at[layer, self.chip, self.core, :, pl.ds(k * WIDE + side, C)], sem).start()
        elif k == 0:
            local(self.wd.at[layer], self.WD.at[layer, self.chip, self.core], sem).start()

    def first(self, u):
        layer, gate, k = self.kind(u)
        mine = self.unit(u, self.chip, self.core)
        if gate:
            self.done(mine, self.wsem.at[0, u])
        elif k == 0:
            self.done(self.WD.at[layer, self.chip, self.core], self.wsem.at[0, u])
        for to in self.planes[:2]:
            self.remote(mine, mine, self.wsem.at[1, u], self.wsem.at[2, u], self.to(to))

    def second(self, u):
        self.done(self.unit(u, 0, pl.ds(0, 2)), self.wsem.at[2, u])
        size = (ROWS if self.kind(u)[1] else PIECE) // 2
        for half in range(2):
            ref = self.unit(u, self.chips[half], self.core, pl.ds(half * size, size))
            self.remote(ref, ref, self.wsem.at[1, u], self.wsem.at[3, u], self.to(self.planes[1 - half]))

    def third(self, u):
        self.done(self.unit(u, 0, 0), self.wsem.at[3, u])
        ref = self.unit(u, slice(None), self.core)
        self.remote(ref, ref, self.wsem.at[5, u], self.wsem.at[4, u], self.to(self.partner))

    def whole(self, u):
        self.done(self.unit(u, slice(None), 0), self.wsem.at[4, u])

    def pass_on(self, it):
        for u in range(2, LAST):
            if (5 * u - 6) // 3 == it:
                self.second(u)
                self.first(u + 2)
        for u in range(1, LAST):
            if 5 * u // 3 == it:
                self.third(u)

    def open(self):
        self.own(1)
        barrier = pltpu.get_barrier_semaphore()
        peers = [self.to(self.partner)] + [self.to(s) for s in self.planes] + [self.to(z=z) for z in self.lines]
        for peer in peers:
            pl.semaphore_signal(barrier, inc=1, device_id=peer, device_id_type=MESH)
        pl.semaphore_wait(barrier, len(peers))
        self.first(0)
        self.first(1)
        for u in range(2, NC + 1):
            self.own(u)

    def weights_first(self):
        self.second(0)
        self.first(2)
        self.second(1)
        self.first(3)
        self.third(0)

    def step0(self, it):
        def case(k):
            self.pass_on(k)
            if k % 2 == 0:
                self.whole(k // 2)
            if PER + k < UNITS:
                self.own(PER + k)

        choose(it, [functools.partial(case, k) for k in range(2 * NC)])

    def step1(self, t):
        def case(k):
            if k == 0:
                self.pass_on(2 * NC)
                self.pass_on(2 * NC + 1)
                for u in range(NC, PER):
                    if 5 * u // 3 >= 2 * NC + 2:
                        self.third(u)
                for u in range(NC, PER):
                    self.whole(u)
            for u in range(PER, LAST):
                if (5 * u - 6) // 3 == k + 2 * NC + 2:
                    self.second(u)
                    self.first(u + 2)
                if 5 * u // 3 == k + 2 * NC + 2:
                    self.third(u)

        choose(t, [functools.partial(case, k) for k in range(NC)])


    @staticmethod
    def scratch():
        blocks, wide = (4, ROWS, WIDE), (ROWS, WIDE)
        return (
            VMEM((2, *blocks), bf16),
            VMEM((SENT, 3, *wide), bf16),
            VMEM((CAME, *wide), f32),
            VMEM((2, LINE, *wide), bf16),
            VMEM((2, *wide), bf16),
            VMEM((2, PIECE, D), bf16),
        )

    def sums(self, ACC, CS, XS, O2, ZS, F, FD):
        self.ACC, self.CS, self.XS, self.O2, self.ZS, self.F, self.FD = ACC, CS, XS, O2, ZS, F, FD

    def free(self, k, to):
        pl.semaphore_signal(self.cred.at[k], inc=1, device_id=to, device_id_type=MESH)

    def pack(self, n, block):
        b = n % 2
        for chip in range(4):
            self.CS[b, chip] = block(2 * chip + 1 - self.core).astype(bf16)

        @pl.when(n >= 2)
        def _():
            pl.semaphore_wait(self.cred.at[0], 1)

        self.remote(self.CS.at[b], self.CR.at[b], self.csem.at[0, b], self.csem.at[1, b], self.to(self.partner))

    def pack_gate(self, n, slot):
        self.pack(n, lambda s: self.ACC[slot, s])

    def plane_gate(self, n, slot):
        self.plane(n, lambda s: self.ACC[slot, s])

    def downs(self, acc, sem):
        self.acc, self.acc_sem = acc, sem
        self.load_down(0)

    def load_down(self, k):
        for b in range(3):
            for h in range(2):
                src = self.dws.at[:, pl.ds(pl.multiple_of(k * PIECE + h * HALF, HALF), HALF), pl.ds(b * C, C)]
                local(src, self.ACC.at[k % 2, :, pl.ds(b * HALF, HALF), pl.ds(h * C, C)], self.acc_sem).start()

    def pack_down1(self, n):
        self.done(self.ACC.at[n % 2], self.acc_sem)
        self.pack_gate(n, n % 2)
        pl.when(n < PER - 1)(lambda: self.load_down(n - NC + 1))

    def down0(self, k):
        def block(s):
            rows = []
            for b in range(3):
                sides = [self.acc[pl.ds(pl.multiple_of(s * C + k * PIECE + h * HALF, HALF), HALF), pl.ds(b * C, C)] for h in range(2)]
                rows.append(jnp.concatenate(sides, 1))
            return jnp.concatenate(rows)

        return block

    def plane(self, n, block):
        b, xs, xb = n % 2, n % SENT, n % CAME
        for side, ref in enumerate((self.CS, self.CR)):
            self.done(ref.at[b], self.csem.at[side, b])

        def total(chip):
            return block(2 * chip + self.core) + self.CR[b, chip].astype(f32)

        for m, chip in enumerate(self.chips):
            self.XS[xs, m] = total(chip).astype(bf16)
        self.O2[xb] = total(self.chip)
        pl.when(n + 2 < UNITS)(lambda: self.free(0, self.to(self.partner)))

        @pl.when(n >= CAME)
        def _():
            for m in OTHERS:
                pl.semaphore_wait(self.cred.at[m], 1)

        for m, s in enumerate(self.planes):
            self.remote(self.XS.at[xs, m], self.XR.at[xb, m], self.xsem.at[0, xs], self.xsem.at[1, xb], self.to(s))

    def line(self, n, k, total):
        zb = n % LINE
        self.ZS[k, zb] = total.astype(bf16)

        @pl.when(n >= LINE)
        def _():
            pl.semaphore_wait(self.cred.at[4 + k], 1)

        self.remote(self.ZS.at[k, zb], self.ZR.at[k, zb], self.zsem.at[k, 0, zb], self.zsem.at[k, 1, zb], self.to(z=self.lines[k]))

    def line_sum(self, n, k):
        zb = n % LINE
        for side, ref in enumerate((self.ZS, self.ZR)):
            self.done(ref.at[k, zb], self.zsem.at[k, side, zb])
        total = self.ZS[k, zb].astype(f32) + self.ZR[k, zb].astype(f32)
        pl.when(n + LINE < UNITS)(lambda: self.free(4 + k, self.to(z=self.lines[k])))
        return total

    def line1(self, n):
        xs, xb = n % SENT, n % CAME
        self.done(self.XS.at[xs], self.xsem.at[0, xs])
        self.done(self.XR.at[xb], self.xsem.at[1, xb])
        total = self.O2[xb] + (self.XR[xb, 0].astype(f32) + self.XR[xb, 1].astype(f32) + self.XR[xb, 2].astype(f32))

        @pl.when(n + CAME < UNITS)
        def _():
            for m, s in zip(OTHERS, self.planes):
                self.free(m, self.to(s))

        self.line(n, 0, total)

    def line2(self, n):
        self.line(n, 1, self.line_sum(n, 0))

    def finish(self, n):
        total = self.line_sum(n, 1).astype(bf16)
        pl.when(n >= 2)(lambda: self.done(self.F.at[n % 2], self.osem.at[n % 2]))
        return total

    def final_gate(self, n, layer, j):
        b = n % 2
        self.F[b] = self.finish(n)
        for side, out in enumerate(self.outs):
            local(self.F.at[b, :, pl.ds(side * C, C)], out.at[layer, :, times(j, C)], self.osem.at[b]).start()

    def final_down(self, n, layer, k):
        b = n % 2
        total = self.finish(n)
        for i in range(3):
            for h in range(2):
                self.FD[b, pl.ds(h * HALF, HALF), pl.ds(i * C, C)] = total[i * HALF : (i + 1) * HALF, h * C : (h + 1) * C]
        local(self.FD.at[b], self.od.at[layer, times(k, PIECE)], self.osem.at[b]).start()

    def final1(self, n):
        self.final_gate(n, 1, n)

    def step2(self, j, t):
        @pl.when(t == 0)
        def _():
            @pl.when(j == 0)
            def _():
                self.third(LAST - 1)
                for u in range(PER, LAST):
                    self.whole(u)

            pl.when(j >= 1)(lambda: self.whole(LAST - 1 + j))
            pl.when(j < UNITS - LAST)(lambda: self.second(LAST + j))
            pl.when(j < UNITS - LAST - 2)(lambda: self.first(LAST + 2 + j))

        @pl.when(t == 1)
        def _():
            pl.when(j < UNITS - LAST)(lambda: self.third(LAST + j))
            pl.when(j >= 1)(lambda: self.plane_gate(j - 1, (j - 1) % 2))
            for back, stage in enumerate((self.line1, self.line2, self.final1), 2):
                pl.when(j >= back)(functools.partial(stage, j - back))

    def end2(self, j):
        self.pack_gate(j, j % 2)

    def step3(self, t):
        pl.when(t <= 3)(lambda: self.final1(4 + t))
        pl.when(t >= 6)(lambda: self.final_down(2 + t, 1, t - 6))
        pl.when(t <= 2)(lambda: self.line2(5 + t))
        pl.when(t >= 4)(lambda: self.line2(4 + t))
        pl.when(t <= 1)(lambda: self.line1(6 + t))
        pl.when((t >= 3) & (t <= 6))(lambda: self.line1(5 + t))
        pl.when(t <= 4)(lambda: self.plane_gate(7 + t, (7 + t) % 2))
        pl.when(t <= 3)(lambda: self.pack_down1(8 + t))

    def step4(self, it):
        pl.when(it <= 1)(lambda: self.final_down(PER - 2 + it, 1, 2 + it))
        pl.when((it == 11) | (it == 14))(lambda: self.final_down(PER + (it - 11) // 3 * 2, 0, (it - 11) // 3))
        pl.when(it == 13)(lambda: self.final_gate(PER + 1, 0, 0))
        for start, stage in ((8, self.line2), (6, self.line1)):
            @pl.when((it >= start) & ((it - start) % 3 != 1))
            def _():
                stage(PER + (2 * (it - start) + 1) // 3)

        @pl.when(it % 2 == 0)
        def _():
            j = it // 2 - 1

            @pl.when((j >= 0) & (j <= 3))
            def _():
                self.plane(PER + it - 2, self.down0(j))
                self.pack_gate(PER + it - 1, j % 2)

            pl.when(j >= 4)(lambda: self.pack_gate(2 * NC + j, j % 2))

        @pl.when(it % 2 == 1)
        def _():
            k = it // 2
            pl.when((k >= 1) & (k <= 4))(lambda: self.plane_gate(PER + it - 2, (k - 1) % 2))
            pl.when(k >= 5)(lambda: self.plane_gate(2 * NC + k - 1, (k - 1) % 2))
            pl.when(k <= 3)(lambda: self.pack(PER + it - 1, self.down0(k)))

    def step5(self, t):
        pl.when((t == 1) | (t == 3))(lambda: self.final_down(PER + 3 + t, 0, (t + 3) // 2))
        pl.when((t == 0) | (t == 2))(lambda: self.final_gate(PER + 3 + t, 0, t // 2 + 1))
        pl.when(t >= 4)(lambda: self.final_gate(PER + 3 + t, 0, t - 1))
        pl.when(t <= 6)(lambda: self.line2(PER + 5 + t))
        pl.when(t <= 4)(lambda: self.line1(PER + 7 + t))
        pl.when(t == 1)(lambda: self.plane_gate(UNITS - 1, 1))
        pl.when(t == 0)(lambda: self.pack_gate(UNITS - 1, 1))

    def close(self):
        self.final_gate(UNITS - 1, 0, NC - 1)
        for b in range(2):
            self.done(self.F.at[b], self.osem.at[b])
        for u in range(UNITS):
            self.done(self.unit(u, pl.ds(0, 3), 0), self.wsem.at[1, u])
            self.done(self.unit(u, slice(None), 0), self.wsem.at[5, u])


def whole(x, dy, wg, wu, wd, dx, og, ou, od, gus, ps, dgus, h1s, a0s, dws, A, DY, WGU, WD, CR, XR, ZR, lsem, wsem, csem, xsem, zsem, osem, cred):
    links = Links(wg, wu, wd, og, ou, od, dws, WGU, WD, CR, XR, ZR, wsem, csem, xsem, zsem, osem, cred)
    kernel(x, dy, wg, wu, wd, dx, og, ou, od, gus, ps, dgus, h1s, a0s, dws, A, DY, WGU, WD, lsem, links)


def hand_out(*refs):
    count = len(refs) // 3
    ins, outs, held, (come, leave) = refs[:count], refs[count : 2 * count], refs[2 * count : 3 * count], refs[3 * count :]
    pieces = [(0, pl.ds(k * N // 4, N // 4)) for k in range(4)] + [(i, slice(None)) for i in range(1, count)]
    arriving = [local(ins[i].at[rows], held[i].at[rows], come.at[k]) for k, (i, rows) in enumerate(pieces)]
    leaving = [local(held[i].at[rows], outs[i].at[rows], leave.at[k]) for k, (i, rows) in enumerate(pieces)]
    for copy in arriving:
        copy.start()
    for first, second in zip(arriving, leaving):
        first.wait()
        second.start()
    arrive(leaving)


def solution(mesh):
    def call(x, dy, wg, wu, wd):
        anywhere = pl.BlockSpec(memory_space=pl.ANY)
        S, V, M = jax.ShapeDtypeStruct, VMEM, SEM
        flops = 17 * 2 * N * D * FF
        out = pl.pallas_call(
            whole,
            in_specs=[anywhere] * 5,
            out_specs=[anywhere] * 10,
            out_shape=[
                S((N, D), bf16),
                S((2, ROWS, FF), bf16),
                S((2, ROWS, FF), bf16),
                S((2, C, D), bf16),
                S((NC, N, WIDE), f32),
                S((N, FF), bf16),
                S((N, BOTH), bf16),
                S((N, D), bf16),
                S((N, D), bf16),
                S((NC, C, D), f32),
            ],
            scratch_shapes=[
                V((N, D), bf16),
                V((N, D), bf16),
                V((2, 4, 2, ROWS, BOTH), bf16),
                V((2, 4, 2, C, D), bf16),
                V((2, 4, ROWS, WIDE), bf16),
                V((CAME, 3, ROWS, WIDE), bf16),
                V((2, LINE, ROWS, WIDE), bf16),
                PAIR,
                M((6, UNITS)),
                M((2, 2)),
                M((2, CAME)),
                M((2, 2, LINE)),
                PAIR,
                pltpu.SemaphoreType.REGULAR((6,)),
            ],
            compiler_params=pltpu.CompilerParams(vmem_limit_bytes=67_000_000, collective_id=0, has_side_effects=True),
            cost_estimate=pl.CostEstimate(flops=flops, bytes_accessed=400_000_000, transcendentals=0),
            name="stack",
        )(x, dy, wg, wu, wd)
        kept = [S(o.shape, bf16) for o in out[:4]]
        return pl.pallas_call(
            hand_out,
            in_specs=[anywhere] * 4,
            out_specs=[anywhere] * 4,
            out_shape=kept,
            scratch_shapes=[V(o.shape, bf16) for o in kept] + [M((7,)), M((7,))],
            compiler_params=pltpu.CompilerParams(vmem_limit_bytes=67_000_000),
            name="hand_out",
        )(*out[:4])

    def step(x, dy, wg, wu, wd):
        dx, *by_weights = call(x[0], dy[0], wg, wu, wd)
        return dx[None], *by_weights

    states, cut = P(("rep", "r", "s"), None, None), P(None, "s", None)
    return jax.shard_map(
        step,
        mesh=mesh,
        in_specs=(states, states) + (cut,) * 3,
        out_specs=(states,) + (P("rep", "s", None),) * 3,
        check_vma=False,
    )
```
